256 devices in a mesh: seq: 64 (over x, z, core), head: 4 (over y).
Axes of the slice: x: 4, y: 4, z: 8, core: 2. Of those that a mesh axis runs over, the one named last changes fastest.
Arguments:
- queries: bfloat16 [16384, 2048], P('seq', 'head'), may hold values from -1.75 to 1.75
- keys: bfloat16 [16384, 2048], P('seq', 'head'), may hold values from -1.75 to 1.75
- values: bfloat16 [16384, 2048], P('seq', 'head'), may hold values from -6 to 6
- level_table: float32 [16, 16], P(None, 'head'), may hold values from 0.05 to 1
- level_code: int32 [16384, 9], P('seq'), may hold values from 0 to 15
- out_weight: bfloat16 [2048, 2048], P('head'), may hold values from -0.125 to 0.125
- cotangent: bfloat16 [16384, 2048], P('seq', 'head'), may hold values from -16 to 16
Outputs:
- mixed: bfloat16 [16384, 2048], P('seq', 'head')
- out_weight_grad: float32 [2048, 2048], P('seq', 'head')
- query_grad: bfloat16 [16384, 2048], P('seq', 'head')
- key_grad: bfloat16 [16384, 2048], P('seq', 'head')
- value_grad: bfloat16 [16384, 2048], P('seq', 'head')
- table_grad: float32 [16, 16], P(None, 'head')
The draws below stay inside these ranges and needn't reach their ends.
All inputs are finite; a program needn't handle non-finite values.
Results may differ from the reference program's by a relative error of at most 0.015.
Values may be sent and summed in bfloat16 or wider, within the bound.
A program may use at most 128 MiB of HBM per device.

```python
import math
import jax
import jax.numpy as jnp
from jax import lax

WIDTH = 2048
HEADS = 16
HEAD_DIM = 128
SPAN = 64
CODES = 16
LEVELS = 9
TOKENS = 16384
N_HEAD = 4


def plant(drawn, stream_key, low, high):
    shape = drawn.shape
    place = [jax.random.randint(jax.random.fold_in(stream_key, axis), (), 0, shape[axis]) for axis in range(len(shape))]
    drawn = drawn.at[tuple(place)].set(low)
    longest = shape.index(max(shape))
    place[longest] = (place[longest] + 1) % shape[longest]
    return drawn.at[tuple(place)].set(high)


def raised(entries, own_key, source, target, blocks, factor):
    def block_of(position):
        return (jnp.arange(entries.shape[position]) // (entries.shape[position] // blocks)).reshape((-1,) + (1,) * (entries.ndim - 1 - position))

    one_side = jax.random.permutation(own_key, blocks)[block_of(target)]
    second = (block_of(target) + blocks // 2) % blocks
    return jnp.where((block_of(source) == one_side) | (block_of(source) == second), factor * entries, entries)


def block_levels(stream_key, extent, split, smallest, high):
    level, own = 1.0, jax.random.fold_in(stream_key, 6)
    for dim, parts in split:
        draws = jnp.exp(jax.random.uniform(jax.random.fold_in(own, dim), (parts,), jnp.float32, smallest / len(split), high / len(split)))
        level = level * jnp.repeat(draws, extent[dim] // parts).reshape([-1 if axis == dim else 1 for axis in range(len(extent))])
    return level


def centred(key, shape, width, limit, shards=(), held_as=jnp.bfloat16):
    drawn = jax.random.normal(key, shape, jnp.float32) * width
    if len(shards) > 0:
        drawn = block_levels(key, shape, shards, -0.22, 0.18) * drawn
    return jnp.clip(drawn, min=-limit, max=limit).astype(held_as)


def noise_with(key, dims, spread, limit, shards, heavy, held_as=jnp.bfloat16):
    values = spread * jax.random.normal(key, dims, jnp.float32)
    if shards:
        values = values * block_levels(key, dims, shards, -0.22, 0.18)
    return jnp.clip(raised(values, jax.random.fold_in(key, 3), *heavy), -limit, limit).astype(held_as)


def setup_inputs(seed: int = 0) -> dict:
    streams_of = jax.random.split(jax.random.key(seed), 8)
    return {
        "queries": centred(streams_of[0], (TOKENS, HEADS * HEAD_DIM), 0.3, 1.75, ((0, 64), (1, 4))),
        "keys": centred(streams_of[1], (TOKENS, HEADS * HEAD_DIM), 0.3, 1.75, ((0, 64), (1, 4))),
        "values": centred(streams_of[2], (TOKENS, HEADS * HEAD_DIM), 1.0, 6.0, ((0, 64), (1, 4))),
        "level_table": jnp.clip(jnp.exp(math.log(1.0) - 2.9957323 * jax.random.uniform(streams_of[3], (CODES, HEADS), jnp.float32) ** block_levels(streams_of[3], (CODES, HEADS), ((1, 4),), -0.2, 0.2)), 0.05, 1.0),
        "level_code": plant(jax.random.randint(streams_of[4], (TOKENS, LEVELS), 0, CODES), jax.random.fold_in(streams_of[4], 1), 0, CODES - 1).astype(jnp.int32),
        "out_weight": centred(streams_of[5], (HEADS * HEAD_DIM, WIDTH), (HEADS * HEAD_DIM) ** -0.5, 0.125, ((0, 4),)),
        "cotangent": noise_with(streams_of[6], (TOKENS, WIDTH), 1.0, 16.0, ((0, 64), (1, 4)), (0, 1, 64, 4.0)),
    }


HIGHEST_PRECISION = lax.Precision.HIGHEST

def level_attention(q_head, k_head, v_head, lam_head):
    span_total = q_head.shape[0] // SPAN
    q_four = q_head.reshape(span_total, SPAN, HEAD_DIM)
    k_four = k_head.reshape(span_total, SPAN, HEAD_DIM)
    v_four = v_head.reshape(span_total, SPAN, HEAD_DIM)
    causal = (jnp.arange(SPAN)[:, None] >= jnp.arange(SPAN)[None, :]).astype(q_head.dtype)
    scores = jnp.einsum('ncd,nsd->ncs', q_four, k_four, precision=HIGHEST_PRECISION) * causal
    within = jnp.einsum('ncs,nse->nce', scores, v_four, precision=HIGHEST_PRECISION).reshape(q_head.shape)
    result = within * (lam_head[:, 0:1] / math.sqrt(SPAN))
    states = jnp.einsum('ncd,nce->nde', k_four, v_four, precision=HIGHEST_PRECISION)
    for bit_index in range(LEVELS - 1):
        group_size = 2 ** (bit_index + 1)
        half_size = group_size // 2
        group_count = span_total // group_size
        lower_state = lax.optimization_barrier(jnp.sum(states.reshape(group_count, group_size, HEAD_DIM, HEAD_DIM)[:, :half_size], axis=1))
        upper_queries = q_four.reshape(group_count, group_size, SPAN, HEAD_DIM)[:, half_size:]
        level_reads = jnp.einsum('gjcd,gde->gjce', upper_queries, lower_state, precision=HIGHEST_PRECISION)
        placed = jnp.concatenate([jnp.zeros_like(level_reads), level_reads], axis=1).reshape(q_head.shape)
        result = result + placed * (lam_head[:, bit_index + 1:bit_index + 2] / math.sqrt(SPAN * 2 ** bit_index))
    return result

def head_major(array):
    return array.reshape(TOKENS, HEADS, HEAD_DIM).transpose(1, 0, 2)

def reference(queries, keys, values, level_table, level_code, out_weight, cotangent):
    lam = jnp.take(level_table, level_code, axis=0)
    lam_heads = jnp.transpose(lam, (2, 0, 1))
    stacked = (head_major(queries), head_major(keys), head_major(values), lam_heads)

    def forward_head(head_items):
        q_head, k_head, v_head, lam_head = head_items
        return level_attention(q_head.astype(jnp.float32), k_head.astype(jnp.float32), v_head.astype(jnp.float32), lam_head)
    attention = lax.map(forward_head, stacked)
    attn_rows = attention.transpose(1, 0, 2).reshape(TOKENS, HEADS * HEAD_DIM).astype(jnp.bfloat16)
    group_cols = HEADS * HEAD_DIM // N_HEAD
    head_total = jnp.zeros((TOKENS, WIDTH), jnp.float32)
    for group_index in range(N_HEAD):
        partial_value = jnp.dot(attn_rows[:, group_index * group_cols:(group_index + 1) * group_cols], out_weight[group_index * group_cols:(group_index + 1) * group_cols], preferred_element_type=jnp.float32)
        head_total = head_total + partial_value.astype(jnp.bfloat16).astype(jnp.float32)
    mixed = head_total.astype(jnp.bfloat16)
    grad_attn = jnp.dot(cotangent, out_weight.T, preferred_element_type=jnp.float32).astype(jnp.bfloat16)
    out_weight_grad = jnp.dot(cotangent.T, attn_rows, preferred_element_type=jnp.float32) / math.sqrt(TOKENS)

    def backward_head(head_items):
        q_head, k_head, v_head, lam_head, grad_head = head_items
        unused, pullback = jax.vjp(level_attention, q_head.astype(jnp.float32), k_head.astype(jnp.float32), v_head.astype(jnp.float32), lam_head)
        return pullback(grad_head.astype(jnp.float32))
    q_grads, k_grads, v_grads, lam_grads = lax.map(backward_head, stacked + (head_major(grad_attn),))

    def rows_back(array):
        return array.transpose(1, 0, 2).reshape(TOKENS, HEADS * HEAD_DIM).astype(jnp.bfloat16)
    one_hot = (level_code[:, :, None] == jnp.arange(CODES, dtype=jnp.int32)[None, None, :]).astype(jnp.float32)
    table_grad = jnp.einsum('htl,tlc->ch', lam_grads, one_hot, precision=HIGHEST_PRECISION) / math.sqrt(TOKENS * LEVELS)
    return (mixed, out_weight_grad, rows_back(q_grads), rows_back(k_grads), rows_back(v_grads), table_grad)
```

```python
import math

import jax
import jax.numpy as jnp
from jax import lax
from jax.experimental import pallas as pl
from jax.experimental.pallas import tpu as pltpu
from jax.sharding import PartitionSpec as P

SPAN = 64
CODES = 16
NX, NZ = 4, 8
F32, BF16 = jnp.float32, jnp.bfloat16
MESH = pl.DeviceIdType.MESH
NN = (((1,), (0,)), ((), ()))
NT = (((1,), (1,)), ((), ()))
TN = (((0,), (0,)), ((), ()))


def mm(left, right, dims):
    return lax.dot_general(left, right, dims, preferred_element_type=F32)


def remote(src, dst, send_sem, recv_sem, device):
    return pltpu.make_async_remote_copy(
        src_ref=src,
        dst_ref=dst,
        send_sem=send_sem,
        recv_sem=recv_sem,
        device_id=device,
        device_id_type=MESH,
    )


def mod(value, size):
    return lax.rem(value + size, size)


def bit_of(value, index):
    return lax.rem(lax.div(value, 2**index), 2)


def kernel(
    q_ref, k_ref, v_ref, table_ref, code_ref, w_ref, cot_ref,
    mixed_ref, wg_ref, qg_ref, kg_ref, vg_ref, tg_ref,
    cotall, coefb, scores, lw, probs, sgbuf, gbuf, abuf, attnl, qgl, kgl, vgl,
    dsend, drecv, zsend_f, zrecv_f, xsend_f, xrecv_f, rsend_f, rx_f, fall,
    t0send, t0recv, tsend, trecv, zsend_b, zrecv_b, xsend_b, xrecv_b, gsend, gall,
    mpart, mrelay, mrecv, wpart, wrecv, wrelay, wxrecv, wz, wzrecv,
    tgsend, tgcore, tgzsend, tgz, tgxsend, tgx,
    cot_s, cot_r, core_s, core_r, zf_s, zf_r, xf_s, xf_r, rf_s, rf_r,
    zb_s, zb_r, xb_s, xb_r, rb_s, rb_r, m_s, m_r, wc_s, wc_r, wx_s, wx_r, wz_s, wz_r,
    tz_s, tz_r, tx_s, tx_r,
):
    s = lax.axis_index("seq")
    y = lax.axis_index("head")
    c = lax.rem(s, 2)
    z = lax.rem(lax.div(s, 2), NZ)
    x = lax.div(s, 2 * NZ)
    other = 1 - c
    heads, size = 4, 128
    rows = q_ref.shape[0]
    half = rows // 2

    def at_y(target):
        return (s, target)

    def at_z(target):
        return ((x * NZ + target) * 2 + c, y)

    def at_x(target):
        return ((target * NZ + z) * 2 + c, y)

    partner = (s + 1 - 2 * c, y)
    level_bits = [bit_of(z, 0), bit_of(z, 1), bit_of(z, 2), bit_of(x, 0), bit_of(x, 1)]
    pending = []

    def go(copy, cond=None):
        pending.append((copy, cond))
        if cond is None:
            copy.start()
        else:
            pl.when(cond)(lambda: copy.start())

    def arrived(dst, sem, cond=None):
        copy = remote(dst, dst, sem, sem, partner)
        if cond is None:
            copy.wait_recv()
        else:
            pl.when(cond)(lambda: copy.wait_recv())

    def col(h):
        return slice(h * size, (h + 1) * size)

    barrier = pltpu.get_barrier_semaphore()
    partners = [partner]
    partners += [at_y(mod(y + off, 4)) for off in range(1, 4)]
    partners += [at_z(mod(z + off, NZ)) for off in range(1, NZ)]
    partners += [at_x(mod(x + off, NX)) for off in range(1, NX)]
    for device in partners:
        pl.semaphore_signal(barrier, inc=1, device_id=device, device_id_type=MESH)

    for h in range(heads):
        dsend[col(h), :] = mm(k_ref[:, col(h)], v_ref[:, col(h)], TN).astype(BF16)
    for l in range(5):
        @pl.when(level_bits[l] == 0)
        def _(l=l):
            fall[l, c] = jnp.zeros((256, size), BF16)
    cotall[y] = cot_ref[...]
    pl.semaphore_wait(barrier, len(partners))

    right, left = mod(y + 1, 4), mod(y - 1, 4)
    top, low = pl.ds(0, half), pl.ds(half, half)
    go(remote(cot_ref.at[top], cotall.at[y, top], cot_s.at[0], cot_r.at[0], at_y(right)))
    go(remote(cot_ref.at[low], cotall.at[y, low], cot_s.at[2], cot_r.at[2], at_y(left)))
    go(remote(cot_ref.at[low], cotall.at[y, low], cot_s.at[1], cot_r.at[1], at_y(right)))
    go(remote(cot_ref.at[top], cotall.at[y, top], cot_s.at[3], cot_r.at[3], at_y(left)))
    go(remote(dsend, drecv, core_s.at[0], core_r.at[0], partner))

    code = code_ref[...]
    levels = code.shape[1]
    lane = lax.broadcasted_iota(jnp.int32, (1, levels), 1)
    scale = jnp.zeros((1, levels), F32)
    scales = [1.0 / math.sqrt(SPAN * 2 ** max(l - 1, 0)) for l in range(levels)]
    for l in range(levels):
        scale = jnp.where(lane == l, scales[l], scale)
    coefs = []
    for h in range(heads):
        lam = jnp.zeros((rows, levels), F32)
        for entry in range(CODES):
            lam = jnp.where(code == entry, table_ref[entry, h], lam)
        coefs.append(lam * scale)

    arrived(drecv, core_r.at[0])
    half_rows = pl.ds(pl.multiple_of(c * 256, 256), 256)
    zsend_f[...] = (dsend[half_rows, :].astype(F32) + drecv[half_rows, :].astype(F32)).astype(BF16)
    for off in range(1, NZ):
        zt = mod(z + off, NZ)
        go(remote(zsend_f.at[pl.ds(pl.multiple_of(zt * 32, 32), 32)], zrecv_f.at[z],
                  zf_s.at[off], zf_r.at[off], at_z(zt)))
    own_slice = pl.ds(pl.multiple_of(z * 32, 32), 32)
    zrecv_f[z] = zsend_f[own_slice, :]

    for h in range(heads):
        for l in range(3, levels):
            coefb[h, l - 3] = jnp.broadcast_to(coefs[h][:, l:l + 1], (rows, size))

    arrived(cotall.at[left, top], cot_r.at[0])
    go(remote(cotall.at[left, top], cotall.at[left, top], cot_s.at[4], cot_r.at[4], at_y(right)))
    arrived(cotall.at[right, low], cot_r.at[2])
    go(remote(cotall.at[right, low], cotall.at[right, low], cot_s.at[5], cot_r.at[5], at_y(left)))

    for off in range(1, NZ):
        arrived(zrecv_f.at[mod(z - off, NZ)], zf_r.at[off])
    parts = [zrecv_f[i].astype(F32) for i in range(NZ)]
    pairs = [parts[2 * i] + parts[2 * i + 1] for i in range(4)]
    quads = [pairs[0] + pairs[1], pairs[2] + pairs[3]]
    xsend_f[...] = (quads[0] + quads[1]).astype(BF16)
    for off in range(1, NX):
        xt = mod(x + off, NX)
        go(remote(xsend_f, xrecv_f.at[x], xf_s.at[off], xf_r.at[off], at_x(xt)), xt > x)
    for zt in range(NZ):
        if zt & 1:
            rsend_f[zt, 0] = parts[zt - 1].astype(BF16)
        if zt & 2:
            rsend_f[zt, 1] = pairs[2 * (zt // 4)].astype(BF16)
        if zt & 4:
            rsend_f[zt, 2] = quads[0].astype(BF16)
    for off in range(1, NZ):
        zt = mod(z + off, NZ)
        for l in range(3):
            go(remote(rsend_f.at[zt, l], fall.at[l, c, own_slice],
                      rf_s.at[off, l], rf_r.at[off, l], at_z(zt)), bit_of(zt, l) == 1)
    for l in range(3):
        @pl.when(level_bits[l] == 1)
        def _(l=l):
            fall[l, c, own_slice, :] = rsend_f[z, l]

    row = lax.broadcasted_iota(jnp.int32, (rows, rows), 0)
    column = lax.broadcasted_iota(jnp.int32, (rows, rows), 1)
    row_span, column_span = row // SPAN, column // SPAN
    in_level = [
        (row_span == column_span) & (column <= row),
        (row_span // 2 == column_span // 2) & (column_span < row_span),
        (row_span >= 2) & (column_span < 2),
    ]
    for h in range(heads):
        weight = jnp.zeros((rows, rows), F32)
        for l in range(3):
            weight = jnp.where(in_level[l], coefs[h][:, l:l + 1], weight)
        score = mm(q_ref[:, col(h)], k_ref[:, col(h)], NT)
        scores[h] = score
        lw[h] = weight
        prob = (score * weight).astype(BF16)
        probs[h] = prob
        attnl[:, col(h)] = mm(prob, v_ref[:, col(h)], NN)

    for off in range(1, NX):
        xs = mod(x - off, NX)
        arrived(xrecv_f.at[xs], xf_r.at[off], xs < x)

    @pl.when(bit_of(x, 0) == 1)
    def _():
        rx_f[0] = xrecv_f[x - 1]
        fall[3, c, own_slice, :] = xrecv_f[x - 1]

    @pl.when(x >= 2)
    def _():
        both = (xrecv_f[0].astype(F32) + xrecv_f[1].astype(F32)).astype(BF16)
        rx_f[1] = both
        fall[4, c, own_slice, :] = both

    for off in range(1, NZ):
        zt = mod(z + off, NZ)
        for l in range(3, 5):
            go(remote(rx_f.at[l - 3], fall.at[l, c, own_slice],
                      rf_s.at[off, l], rf_r.at[off, l], at_z(zt)), level_bits[l] == 1)

    opposite = mod(y + 2, 4)
    arrived(cotall.at[left, low], cot_r.at[1])
    arrived(cotall.at[right, top], cot_r.at[3])
    arrived(cotall.at[opposite, top], cot_r.at[4])
    arrived(cotall.at[opposite, low], cot_r.at[5])
    full_rows = jnp.concatenate([cotall[i] for i in range(4)], axis=1)
    gbuf[...] = mm(full_rows, w_ref[...], NT).astype(BF16)

    for h in range(heads):
        grad = gbuf[:, col(h)].astype(F32)
        for l in range(6):
            sgbuf[h, :, col(l)] = (coefb[h, l] * grad).astype(BF16)
        terms = mm(q_ref[:, col(h)], sgbuf[h], TN)
        t0send[col(h), :] = terms[:, col(0)].astype(BF16)
        for l in range(5):
            tsend[l, h // 2, col(h % 2), :] = terms[:, col(l + 1)].astype(BF16)
    go(remote(tsend.at[:, other], trecv, core_s.at[1], core_r.at[1], partner))
    go(remote(t0send, t0recv, core_s.at[2], core_r.at[2], partner))

    code_f = code.astype(F32)
    wide = jnp.concatenate([code_f, jnp.zeros((rows, size - levels), F32)], axis=1)
    code_t = wide.T
    entry_row = lax.broadcasted_iota(jnp.int32, (CODES, rows), 0).astype(F32)
    one_hot = [
        jnp.where(jnp.broadcast_to(code_t[l:l + 1, :], (CODES, rows)) == entry_row, 1.0, 0.0).astype(BF16)
        for l in range(levels)
    ]
    table_parts = []

    def local_back(h):
        grad = gbuf[:, col(h)]
        prob_grad = mm(grad, v_ref[:, col(h)], NT)
        score_grad = (prob_grad * lw[h]).astype(BF16)
        product = scores[h] * prob_grad
        total = jnp.zeros((CODES, rows), F32)
        for l in range(3):
            masked = jnp.where(in_level[l], product, 0.0).astype(BF16)
            total = total + scales[l] * mm(one_hot[l], masked, NN)
        table_parts.append(total[:, :size] + total[:, size:])
        qgl[:, col(h)] = mm(score_grad, k_ref[:, col(h)], NN)
        kgl[:, col(h)] = mm(score_grad, q_ref[:, col(h)], TN)
        vgl[:, col(h)] = mm(probs[h], grad, TN)

    for h in range(2):
        local_back(h)

    arrived(trecv, core_r.at[1])
    for l in range(5):
        zsend_b[l] = (tsend[l, c].astype(F32) + trecv[l].astype(F32)).astype(BF16)
    for off in range(1, NZ):
        zt = mod(z + off, NZ)
        for l in range(5):
            go(remote(zsend_b.at[l, pl.ds(pl.multiple_of(zt * 32, 32), 32)], zrecv_b.at[z, l],
                      zb_s.at[off, l], zb_r.at[off, l], at_z(zt)), level_bits[l] == 1)
    for l in range(5):
        @pl.when(level_bits[l] == 1)
        def _(l=l):
            zrecv_b[z, l] = zsend_b[l, own_slice, :]

    for off in range(1, NZ):
        zs = mod(z - off, NZ)
        zs_slice = pl.ds(pl.multiple_of(zs * 32, 32), 32)
        for l in range(5):
            arrived(fall.at[l, c, zs_slice], rf_r.at[off, l], level_bits[l] == 1)
    go(remote(fall.at[:, c], fall.at[:, c], core_s.at[3], core_r.at[3], partner))

    for h in range(2, heads):
        local_back(h)

    arrived(fall.at[:, other], core_r.at[3])

    for h in range(heads):
        query, grad = q_ref[:, col(h)], gbuf[:, col(h)].astype(F32)
        found = [jnp.where(c == 1, drecv[col(h), :], jnp.zeros((size, size), BF16))]
        found += [fall[l, h // 2, col(h % 2), :] for l in range(5)]
        found = jnp.concatenate(found, axis=1)
        reads = mm(query, found, NN)
        attention = attnl[:, col(h)]
        total = table_parts[h]
        for l in range(6):
            read = reads[:, col(l)]
            attention = attention + coefb[h, l] * read
            total = total + scales[l + 3] * mm(one_hot[l + 3], (grad * read).astype(BF16), NN)
        table_parts[h] = total
        abuf[:, col(h)] = attention.astype(BF16)
        qg_ref[:, col(h)] = (qgl[:, col(h)] + mm(sgbuf[h], found, NT)).astype(BF16)

    def product_for(target):
        columns = pl.ds(pl.multiple_of(target * 512, 512), 512)
        mpart[target] = mm(abuf[...], w_ref[:, columns], NN).astype(BF16)

    product_for(opposite)
    go(remote(mpart.at[opposite, top], mrelay.at[0], m_s.at[0], m_r.at[0], at_y(left)))
    go(remote(mpart.at[opposite, low], mrelay.at[1], m_s.at[1], m_r.at[1], at_y(right)))

    x_right, x_left, x_opposite = mod(x + 1, 4), mod(x - 1, 4), mod(x + 2, 4)

    def weight_part(step, target):
        part = mm(cotall[target], abuf[...], TN)
        for block in range(16):
            wpart[target, block % 2, pl.ds((block // 2) * 32, 32), :] = (
                part[block * 32:(block + 1) * 32].astype(BF16)
            )
        go(remote(wpart.at[target, other], wrecv.at[target], wc_s.at[step], wc_r.at[step], partner))

    weight_part(0, x_opposite)
    product_for(left)
    product_for(right)
    weight_part(1, x_left)

    def weight_chip(step, target):
        arrived(wrecv.at[target], wc_r.at[step])
        wpart[target, c] = (wpart[target, c].astype(F32) + wrecv[target].astype(F32)).astype(BF16)

    weight_chip(0, x_opposite)
    go(remote(wpart.at[x_opposite, c, top], wrelay.at[0], wx_s.at[0], wx_r.at[0], at_x(x_left)))
    go(remote(wpart.at[x_opposite, c, low], wrelay.at[1], wx_s.at[1], wx_r.at[1], at_x(x_right)))

    arrived(mrelay.at[0], m_r.at[0])
    mpart[left, top] = (mpart[left, top].astype(F32) + mrelay[0].astype(F32)).astype(BF16)
    go(remote(mpart.at[left], mrecv.at[0], m_s.at[2], m_r.at[2], at_y(left)))
    arrived(mrelay.at[1], m_r.at[1])
    mpart[right, low] = (mpart[right, low].astype(F32) + mrelay[1].astype(F32)).astype(BF16)
    go(remote(mpart.at[right], mrecv.at[1], m_s.at[3], m_r.at[3], at_y(right)))

    weight_part(2, x_right)
    weight_part(3, x)
    product_for(y)

    lane128 = lax.broadcasted_iota(jnp.int32, (CODES, size), 1)
    partial_table = jnp.zeros((CODES, size), F32)
    for h in range(heads):
        summed = jnp.sum(table_parts[h], axis=1, keepdims=True)
        partial_table = jnp.where(lane128 == h, summed, partial_table)
    tgsend[...] = partial_table
    go(remote(tgsend, tgcore, core_s.at[4], core_r.at[4], partner))

    for off in range(1, NZ):
        zs = mod(z - off, NZ)
        for l in range(5):
            bit = bit_of(zs, l) if l < 3 else level_bits[l]
            arrived(zrecv_b.at[zs, l], zb_r.at[off, l], bit == 1)
    for l in range(2):
        @pl.when(level_bits[3 + l] == 1)
        def _(l=l):
            ring = zrecv_b[0, 3 + l].astype(F32)
            for zs in range(1, NZ):
                ring = ring + zrecv_b[zs, 3 + l].astype(F32)
            xsend_b[l] = ring.astype(BF16)
    for off in range(1, NX):
        xt = mod(x + off, NX)
        bit = jnp.where(lax.div(x, 2) == lax.div(xt, 2), 0, 1)
        go(remote(xsend_b.at[bit], xrecv_b.at[x], xb_s.at[off], xb_r.at[off], at_x(xt)), xt < x)

    weight_chip(1, x_left)
    weight_chip(2, x_right)
    arrived(wrelay.at[0], wx_r.at[0])
    wpart[x_left, c, top] = (wpart[x_left, c, top].astype(F32) + wrelay[0].astype(F32)).astype(BF16)
    go(remote(wpart.at[x_left, c], wxrecv.at[0], wx_s.at[2], wx_r.at[2], at_x(x_left)))
    arrived(wrelay.at[1], wx_r.at[1])
    wpart[x_right, c, low] = (wpart[x_right, c, low].astype(F32) + wrelay[1].astype(F32)).astype(BF16)
    go(remote(wpart.at[x_right, c], wxrecv.at[1], wx_s.at[3], wx_r.at[3], at_x(x_right)))

    arrived(tgcore, core_r.at[4])
    tgzsend[...] = tgsend[...] + tgcore[...]
    for off in range(1, NZ):
        go(remote(tgzsend, tgz.at[z], tz_s.at[off], tz_r.at[off], at_z(mod(z + off, NZ))))
    tgz[z] = tgzsend[...]

    for off in range(1, NX):
        xs = mod(x - off, NX)
        arrived(xrecv_b.at[xs], xb_r.at[off], xs > x)
    from_x = jnp.zeros((32, size), F32)
    for xs in range(1, NX):
        from_x = from_x + jnp.where(x < xs, xrecv_b[xs].astype(F32), 0.0)
    quad = zrecv_b[4, 2].astype(F32)
    for zs in range(5, NZ):
        quad = quad + zrecv_b[zs, 2].astype(F32)
    for zt in range(NZ):
        total = from_x
        if zt & 1 == 0:
            total = total + zrecv_b[zt + 1, 0].astype(F32)
        if zt & 2 == 0:
            upper = (zt // 4) * 4 + 2
            total = total + zrecv_b[upper, 1].astype(F32) + zrecv_b[upper + 1, 1].astype(F32)
        if zt & 4 == 0:
            total = total + quad
        gsend[zt] = total.astype(BF16)
    for off in range(1, NZ):
        zt = mod(z + off, NZ)
        go(remote(gsend.at[zt], gall.at[c, own_slice], rb_s.at[off], rb_r.at[off], at_z(zt)))
    gall[c, own_slice, :] = gsend[z]

    weight_chip(3, x)

    for off in range(1, NZ):
        zs = mod(z - off, NZ)
        arrived(gall.at[c, pl.ds(pl.multiple_of(zs * 32, 32), 32)], rb_r.at[off])
    go(remote(gall.at[c], gall.at[c], core_s.at[5], core_r.at[5], partner))

    arrived(wxrecv.at[0], wx_r.at[2])
    arrived(wxrecv.at[1], wx_r.at[3])
    wz[...] = (
        wpart[x, c].astype(F32) + wxrecv[0].astype(F32) + wxrecv[1].astype(F32)
    ).astype(BF16)
    for off in range(1, NZ):
        zt = mod(z + off, NZ)
        go(remote(wz.at[pl.ds(pl.multiple_of(zt * 32, 32), 32)], wzrecv.at[z],
                  wz_s.at[off], wz_r.at[off], at_z(zt)))
    wzrecv[z] = wz[own_slice, :]

    for off in range(1, NZ):
        arrived(tgz.at[mod(z - off, NZ)], tz_r.at[off])
    ring_table = tgz[0]
    for zs in range(1, NZ):
        ring_table = ring_table + tgz[zs]
    tgxsend[...] = ring_table
    for off in range(1, NX):
        go(remote(tgxsend, tgx.at[x], tx_s.at[off], tx_r.at[off], at_x(mod(x + off, NX))))
    tgx[x] = ring_table

    arrived(gall.at[other], core_r.at[5])
    arrived(t0recv, core_r.at[2])
    for h in range(heads):
        back = gall[h // 2, col(h % 2), :].astype(F32) + jnp.where(c == 0, t0recv[col(h), :].astype(F32), 0.0)
        back = back.astype(BF16)
        kg_ref[:, col(h)] = (kgl[:, col(h)] + mm(v_ref[:, col(h)], back, NT)).astype(BF16)
        vg_ref[:, col(h)] = (vgl[:, col(h)] + mm(k_ref[:, col(h)], back, NN)).astype(BF16)

    arrived(mrecv.at[0], m_r.at[2])
    arrived(mrecv.at[1], m_r.at[3])
    mixed_ref[...] = (
        mpart[y].astype(F32) + mrecv[0].astype(F32) + mrecv[1].astype(F32)
    ).astype(BF16)

    for off in range(1, NX):
        arrived(tgx.at[mod(x - off, NX)], tx_r.at[off])
    table = tgx[0]
    for xs in range(1, NX):
        table = table + tgx[xs]
    tokens = rows * 2 * NZ * NX
    tg_ref[...] = table[:, :heads] * (1.0 / math.sqrt(tokens * levels))

    for off in range(1, NZ):
        arrived(wzrecv.at[mod(z - off, NZ)], wz_r.at[off])
    weight = wzrecv[0].astype(F32)
    for zs in range(1, NZ):
        weight = weight + wzrecv[zs].astype(F32)
    wg_ref[...] = weight * (1.0 / math.sqrt(tokens))

    for copy, cond in pending:
        if cond is None:
            copy.wait_send()
        else:
            pl.when(cond)(lambda copy=copy: copy.wait_send())


def per_device(queries, keys, values, level_table, level_code, out_weight, cotangent):
    rows, width = queries.shape
    vmem = pl.BlockSpec(memory_space=pltpu.VMEM)
    smem = pl.BlockSpec(memory_space=pltpu.SMEM)
    dma = pltpu.SemaphoreType.DMA

    def bf(*shape):
        return pltpu.VMEM(shape, BF16)

    def f32(*shape):
        return pltpu.VMEM(shape, F32)

    scratch = [
        bf(4, rows, 512), f32(4, 6, rows, 128), f32(4, rows, rows), f32(4, rows, rows),
        bf(4, rows, rows), bf(4, rows, 768), bf(rows, 512), bf(rows, 512),
        f32(rows, 512), f32(rows, 512), f32(rows, 512), f32(rows, 512),
        bf(512, 128), bf(512, 128), bf(256, 128), bf(NZ, 32, 128), bf(32, 128), bf(NX, 32, 128),
        bf(NZ, 3, 32, 128), bf(2, 32, 128), bf(5, 2, 256, 128),
        bf(512, 128), bf(512, 128), bf(5, 2, 256, 128), bf(5, 256, 128), bf(5, 256, 128),
        bf(NZ, 5, 32, 128), bf(2, 32, 128), bf(NX, 32, 128), bf(NZ, 32, 128), bf(2, 256, 128),
        bf(4, rows, 512), bf(2, rows // 2, 512), bf(2, rows, 512),
        bf(4, 2, 256, 512), bf(4, 256, 512), bf(2, 128, 512), bf(2, 256, 512), bf(256, 512),
        bf(NZ, 32, 512),
        f32(CODES, 128), f32(CODES, 128), f32(CODES, 128), f32(NZ, CODES, 128),
        f32(CODES, 128), f32(NX, CODES, 128),
        dma((6,)), dma((6,)), dma((6,)), dma((6,)), dma((NZ,)), dma((NZ,)), dma((NX,)), dma((NX,)),
        dma((NZ, 5)), dma((NZ, 5)), dma((NZ, 5)), dma((NZ, 5)), dma((NX,)), dma((NX,)),
        dma((NZ,)), dma((NZ,)), dma((4,)), dma((4,)), dma((4,)), dma((4,)), dma((4,)), dma((4,)),
        dma((NZ,)), dma((NZ,)), dma((NZ,)), dma((NZ,)), dma((NX,)), dma((NX,)),
    ]
    shape = jax.ShapeDtypeStruct
    return pl.pallas_call(
        kernel,
        out_shape=(
            shape((rows, width), BF16),
            shape((32, width), F32),
            shape((rows, width), BF16),
            shape((rows, width), BF16),
            shape((rows, width), BF16),
            shape((CODES, 4), F32),
        ),
        in_specs=[vmem, vmem, vmem, smem, vmem, vmem, vmem],
        out_specs=[vmem] * 6,
        scratch_shapes=scratch,
        compiler_params=pltpu.CompilerParams(
            collective_id=0, has_side_effects=True, vmem_limit_bytes=56 * 2**20
        ),
        name="layer",
    )(queries, keys, values, level_table, level_code, out_weight, cotangent)


def solution(mesh):
    wide = P("seq", "head")
    return jax.shard_map(
        per_device,
        mesh=mesh,
        in_specs=(wide, wide, wide, P(None, "head"), P("seq", None), P("head", None), wide),
        out_specs=(wide, wide, wide, wide, wide, P(None, "head")),
        check_vma=False,
    )
```

```python
import math

import jax
import jax.numpy as jnp
from jax import lax
from jax.experimental import pallas as pl
from jax.experimental.pallas import tpu as pltpu
from jax.sharding import PartitionSpec as P

SPAN = 64
CODES = 16
NX, NZ = 4, 8
F32, BF16 = jnp.float32, jnp.bfloat16
MESH = pl.DeviceIdType.MESH
NN = (((1,), (0,)), ((), ()))
NT = (((1,), (1,)), ((), ()))
TN = (((0,), (0,)), ((), ()))


def mm(left, right, dims):
    return lax.dot_general(left, right, dims, preferred_element_type=F32)


def remote(src, dst, send_sem, recv_sem, device):
    return pltpu.make_async_remote_copy(
        src_ref=src,
        dst_ref=dst,
        send_sem=send_sem,
        recv_sem=recv_sem,
        device_id=device,
        device_id_type=MESH,
    )


def mod(value, size):
    return lax.rem(value + size, size)


def bit_of(value, index):
    return lax.rem(lax.div(value, 2**index), 2)


def kernel(
    q_hbm, k_hbm, v_hbm, table_ref, code_ref, w_hbm, cot_hbm,
    mixed_ref, wg_ref, qg_ref, kg_ref, vg_ref, tg_ref,
    q_ref, k_ref, v_ref, w_ref, load_sems, cotall, coefb, scores, lw, probs, sgbuf, gbuf, abuf, attnl, qgl, kgl, vgl,
    dsend, drecv, zsend_f, zrecv_f, xsend_f, xrecv_f, rsend_f, rx_f, fall,
    t0send, t0recv, tsend, trecv, zsend_b, zrecv_b, xsend_b, xrecv_b, gsend, gall,
    mpart, mrelay, mrecv, wpart, wrecv, wrelay, wxrecv, wz, wzrecv,
    tgsend, tgcore, tgzsend, tgz, tgxsend, tgx,
    cot_s, cot_r, core_s, core_r, zf_s, zf_r, xf_s, xf_r, rf_s, rf_r,
    zb_s, zb_r, xb_s, xb_r, rb_s, rb_r, m_s, m_r, wc_s, wc_r, wx_s, wx_r, wz_s, wz_r,
    tz_s, tz_r, tx_s, tx_r,
):
    s = lax.axis_index("seq")
    y = lax.axis_index("head")
    c = lax.rem(s, 2)
    z = lax.rem(lax.div(s, 2), NZ)
    x = lax.div(s, 2 * NZ)
    other = 1 - c
    heads, size = 4, 128
    rows = q_ref.shape[0]
    loads = [
        pltpu.make_async_copy(source, target, load_sems.at[i])
        for i, (source, target) in enumerate(
            [(cot_hbm, cotall.at[y]), (k_hbm, k_ref), (v_hbm, v_ref), (q_hbm, q_ref), (w_hbm, w_ref)]
        )
    ]
    for load in loads:
        load.start()
    half = rows // 2

    def at_y(target):
        return (s, target)

    def at_z(target):
        return ((x * NZ + target) * 2 + c, y)

    def at_x(target):
        return ((target * NZ + z) * 2 + c, y)

    partner = (s + 1 - 2 * c, y)
    level_bits = [bit_of(z, 0), bit_of(z, 1), bit_of(z, 2), bit_of(x, 0), bit_of(x, 1)]
    pending = []

    def go(copy, cond=None):
        pending.append((copy, cond))
        if cond is None:
            copy.start()
        else:
            pl.when(cond)(lambda: copy.start())

    def arrived(dst, sem, cond=None):
        copy = remote(dst, dst, sem, sem, partner)
        if cond is None:
            copy.wait_recv()
        else:
            pl.when(cond)(lambda: copy.wait_recv())

    def col(h):
        return slice(h * size, (h + 1) * size)

    barrier = pltpu.get_barrier_semaphore()
    partners = [partner]
    partners += [at_y(mod(y + off, 4)) for off in range(1, 4)]
    partners += [at_z(mod(z + off, NZ)) for off in range(1, NZ)]
    partners += [at_x(mod(x + off, NX)) for off in range(1, NX)]
    for device in partners:
        pl.semaphore_signal(barrier, inc=1, device_id=device, device_id_type=MESH)

    loads[1].wait()
    loads[2].wait()
    for h in range(heads):
        dsend[col(h), :] = mm(k_ref[:, col(h)], v_ref[:, col(h)], TN).astype(BF16)
    for l in range(5):
        @pl.when(level_bits[l] == 0)
        def _(l=l):
            fall[l, c] = jnp.zeros((256, size), BF16)
    loads[0].wait()
    pl.semaphore_wait(barrier, len(partners))

    right, left = mod(y + 1, 4), mod(y - 1, 4)
    top, low = pl.ds(0, half), pl.ds(half, half)
    go(remote(cotall.at[y, top], cotall.at[y, top], cot_s.at[0], cot_r.at[0], at_y(right)))
    go(remote(cotall.at[y, low], cotall.at[y, low], cot_s.at[2], cot_r.at[2], at_y(left)))
    go(remote(cotall.at[y, low], cotall.at[y, low], cot_s.at[1], cot_r.at[1], at_y(right)))
    go(remote(cotall.at[y, top], cotall.at[y, top], cot_s.at[3], cot_r.at[3], at_y(left)))
    go(remote(dsend, drecv, core_s.at[0], core_r.at[0], partner))

    levels = code_ref.shape[0]
    code_t = code_ref[...].astype(F32)
    padding = jnp.zeros((size - levels, rows), F32)
    code = jnp.concatenate([code_t, padding], axis=0).T
    lane = lax.broadcasted_iota(jnp.int32, (1, size), 1)
    scale = jnp.zeros((1, size), F32)
    scales = [1.0 / math.sqrt(SPAN * 2 ** max(l - 1, 0)) for l in range(levels)]
    for l in range(levels):
        scale = jnp.where(lane == l, scales[l], scale)
    coefs = []
    for h in range(heads):
        lam = jnp.zeros((rows, size), F32)
        for entry in range(CODES):
            lam = jnp.where(code == float(entry), table_ref[h, entry], lam)
        coefs.append(lam * scale)

    arrived(drecv, core_r.at[0])
    half_rows = pl.ds(pl.multiple_of(c * 256, 256), 256)
    zsend_f[...] = (dsend[half_rows, :].astype(F32) + drecv[half_rows, :].astype(F32)).astype(BF16)
    for off in range(1, NZ):
        zt = mod(z + off, NZ)
        go(remote(zsend_f.at[pl.ds(pl.multiple_of(zt * 32, 32), 32)], zrecv_f.at[z],
                  zf_s.at[off], zf_r.at[off], at_z(zt)))
    own_slice = pl.ds(pl.multiple_of(z * 32, 32), 32)
    zrecv_f[z] = zsend_f[own_slice, :]

    for h in range(heads):
        for l in range(3, levels):
            coefb[h, l - 3] = jnp.broadcast_to(coefs[h][:, l:l + 1], (rows, size))

    arrived(cotall.at[left, top], cot_r.at[0])
    go(remote(cotall.at[left, top], cotall.at[left, top], cot_s.at[4], cot_r.at[4], at_y(right)))
    arrived(cotall.at[right, low], cot_r.at[2])
    go(remote(cotall.at[right, low], cotall.at[right, low], cot_s.at[5], cot_r.at[5], at_y(left)))

    for off in range(1, NZ):
        arrived(zrecv_f.at[mod(z - off, NZ)], zf_r.at[off])
    parts = [zrecv_f[i].astype(F32) for i in range(NZ)]
    pairs = [parts[2 * i] + parts[2 * i + 1] for i in range(4)]
    quads = [pairs[0] + pairs[1], pairs[2] + pairs[3]]
    xsend_f[...] = (quads[0] + quads[1]).astype(BF16)
    for off in range(1, NX):
        xt = mod(x + off, NX)
        go(remote(xsend_f, xrecv_f.at[x], xf_s.at[off], xf_r.at[off], at_x(xt)), xt > x)
    for zt in range(NZ):
        if zt & 1:
            rsend_f[zt, 0] = parts[zt - 1].astype(BF16)
        if zt & 2:
            rsend_f[zt, 1] = pairs[2 * (zt // 4)].astype(BF16)
        if zt & 4:
            rsend_f[zt, 2] = quads[0].astype(BF16)
    for off in range(1, NZ):
        zt = mod(z + off, NZ)
        for l in range(3):
            go(remote(rsend_f.at[zt, l], fall.at[l, c, own_slice],
                      rf_s.at[off, l], rf_r.at[off, l], at_z(zt)), bit_of(zt, l) == 1)
    for l in range(3):
        @pl.when(level_bits[l] == 1)
        def _(l=l):
            fall[l, c, own_slice, :] = rsend_f[z, l]

    loads[3].wait()
    row = lax.broadcasted_iota(jnp.int32, (rows, rows), 0)
    column = lax.broadcasted_iota(jnp.int32, (rows, rows), 1)
    row_span, column_span = row // SPAN, column // SPAN
    in_level = [
        (row_span == column_span) & (column <= row),
        (row_span // 2 == column_span // 2) & (column_span < row_span),
        (row_span >= 2) & (column_span < 2),
    ]
    for h in range(heads):
        weight = jnp.zeros((rows, rows), F32)
        for l in range(3):
            weight = jnp.where(in_level[l], coefs[h][:, l:l + 1], weight)
        score = mm(q_ref[:, col(h)], k_ref[:, col(h)], NT)
        scores[h] = score
        lw[h] = weight
        prob = (score * weight).astype(BF16)
        probs[h] = prob
        attnl[:, col(h)] = mm(prob, v_ref[:, col(h)], NN)

    for off in range(1, NX):
        xs = mod(x - off, NX)
        arrived(xrecv_f.at[xs], xf_r.at[off], xs < x)

    @pl.when(bit_of(x, 0) == 1)
    def _():
        rx_f[0] = xrecv_f[x - 1]
        fall[3, c, own_slice, :] = xrecv_f[x - 1]

    @pl.when(x >= 2)
    def _():
        both = (xrecv_f[0].astype(F32) + xrecv_f[1].astype(F32)).astype(BF16)
        rx_f[1] = both
        fall[4, c, own_slice, :] = both

    for off in range(1, NZ):
        zt = mod(z + off, NZ)
        for l in range(3, 5):
            go(remote(rx_f.at[l - 3], fall.at[l, c, own_slice],
                      rf_s.at[off, l], rf_r.at[off, l], at_z(zt)), level_bits[l] == 1)

    loads[4].wait()
    opposite = mod(y + 2, 4)
    arrived(cotall.at[left, low], cot_r.at[1])
    arrived(cotall.at[right, top], cot_r.at[3])
    arrived(cotall.at[opposite, top], cot_r.at[4])
    arrived(cotall.at[opposite, low], cot_r.at[5])
    full_rows = jnp.concatenate([cotall[i] for i in range(4)], axis=1)
    gbuf[...] = mm(full_rows, w_ref[...], NT).astype(BF16)

    for h in range(heads):
        grad = gbuf[:, col(h)].astype(F32)
        for l in range(6):
            sgbuf[h, :, col(l)] = (coefb[h, l] * grad).astype(BF16)
        terms = mm(q_ref[:, col(h)], sgbuf[h], TN)
        t0send[col(h), :] = terms[:, col(0)].astype(BF16)
        for l in range(5):
            tsend[l, h // 2, col(h % 2), :] = terms[:, col(l + 1)].astype(BF16)
    go(remote(tsend.at[:, other], trecv, core_s.at[1], core_r.at[1], partner))
    go(remote(t0send, t0recv, core_s.at[2], core_r.at[2], partner))

    entry_row = lax.broadcasted_iota(jnp.int32, (CODES, rows), 0).astype(F32)
    one_hot = [
        jnp.where(jnp.broadcast_to(code_t[l:l + 1, :], (CODES, rows)) == entry_row, 1.0, 0.0).astype(BF16)
        for l in range(levels)
    ]
    table_parts = []

    def local_back(h):
        grad = gbuf[:, col(h)]
        prob_grad = mm(grad, v_ref[:, col(h)], NT)
        score_grad = (prob_grad * lw[h]).astype(BF16)
        product = scores[h] * prob_grad
        total = jnp.zeros((CODES, rows), F32)
        for l in range(3):
            masked = jnp.where(in_level[l], product, 0.0).astype(BF16)
            total = total + scales[l] * mm(one_hot[l], masked, NN)
        table_parts.append(total[:, :size] + total[:, size:])
        qgl[:, col(h)] = mm(score_grad, k_ref[:, col(h)], NN)
        kgl[:, col(h)] = mm(score_grad, q_ref[:, col(h)], TN)
        vgl[:, col(h)] = mm(probs[h], grad, TN)

    for h in range(2):
        local_back(h)

    arrived(trecv, core_r.at[1])
    for l in range(5):
        zsend_b[l] = (tsend[l, c].astype(F32) + trecv[l].astype(F32)).astype(BF16)
    for off in range(1, NZ):
        zt = mod(z + off, NZ)
        for l in range(5):
            go(remote(zsend_b.at[l, pl.ds(pl.multiple_of(zt * 32, 32), 32)], zrecv_b.at[z, l],
                      zb_s.at[off, l], zb_r.at[off, l], at_z(zt)), level_bits[l] == 1)
    for l in range(5):
        @pl.when(level_bits[l] == 1)
        def _(l=l):
            zrecv_b[z, l] = zsend_b[l, own_slice, :]

    for off in range(1, NZ):
        zs = mod(z - off, NZ)
        zs_slice = pl.ds(pl.multiple_of(zs * 32, 32), 32)
        for l in range(5):
            arrived(fall.at[l, c, zs_slice], rf_r.at[off, l], level_bits[l] == 1)
    go(remote(fall.at[:, c], fall.at[:, c], core_s.at[3], core_r.at[3], partner))

    for h in range(2, heads):
        local_back(h)

    arrived(fall.at[:, other], core_r.at[3])

    for h in range(heads):
        query, grad = q_ref[:, col(h)], gbuf[:, col(h)].astype(F32)
        found = [jnp.where(c == 1, drecv[col(h), :], jnp.zeros((size, size), BF16))]
        found += [fall[l, h // 2, col(h % 2), :] for l in range(5)]
        found = jnp.concatenate(found, axis=1)
        reads = mm(query, found, NN)
        attention = attnl[:, col(h)]
        total = table_parts[h]
        for l in range(6):
            read = reads[:, col(l)]
            attention = attention + coefb[h, l] * read
            total = total + scales[l + 3] * mm(one_hot[l + 3], (grad * read).astype(BF16), NN)
        table_parts[h] = total
        abuf[:, col(h)] = attention.astype(BF16)
        qg_ref[:, col(h)] = (qgl[:, col(h)] + mm(sgbuf[h], found, NT)).astype(BF16)

    def product_for(target):
        columns = pl.ds(pl.multiple_of(target * 512, 512), 512)
        mpart[target] = mm(abuf[...], w_ref[:, columns], NN).astype(BF16)

    product_for(opposite)
    go(remote(mpart.at[opposite, top], mrelay.at[0], m_s.at[0], m_r.at[0], at_y(left)))
    go(remote(mpart.at[opposite, low], mrelay.at[1], m_s.at[1], m_r.at[1], at_y(right)))

    x_right, x_left, x_opposite = mod(x + 1, 4), mod(x - 1, 4), mod(x + 2, 4)

    def weight_part(step, target):
        part = mm(cotall[target], abuf[...], TN)
        for block in range(16):
            wpart[target, block % 2, pl.ds((block // 2) * 32, 32), :] = (
                part[block * 32:(block + 1) * 32].astype(BF16)
            )
        go(remote(wpart.at[target, other], wrecv.at[target], wc_s.at[step], wc_r.at[step], partner))

    weight_part(0, x_opposite)
    product_for(left)
    product_for(right)
    weight_part(1, x_left)

    def weight_chip(step, target):
        arrived(wrecv.at[target], wc_r.at[step])
        wpart[target, c] = (wpart[target, c].astype(F32) + wrecv[target].astype(F32)).astype(BF16)

    weight_chip(0, x_opposite)
    go(remote(wpart.at[x_opposite, c, top], wrelay.at[0], wx_s.at[0], wx_r.at[0], at_x(x_left)))
    go(remote(wpart.at[x_opposite, c, low], wrelay.at[1], wx_s.at[1], wx_r.at[1], at_x(x_right)))

    arrived(mrelay.at[0], m_r.at[0])
    mpart[left, top] = (mpart[left, top].astype(F32) + mrelay[0].astype(F32)).astype(BF16)
    go(remote(mpart.at[left], mrecv.at[0], m_s.at[2], m_r.at[2], at_y(left)))
    arrived(mrelay.at[1], m_r.at[1])
    mpart[right, low] = (mpart[right, low].astype(F32) + mrelay[1].astype(F32)).astype(BF16)
    go(remote(mpart.at[right], mrecv.at[1], m_s.at[3], m_r.at[3], at_y(right)))

    weight_part(2, x_right)
    weight_part(3, x)
    product_for(y)

    lane128 = lax.broadcasted_iota(jnp.int32, (CODES, size), 1)
    partial_table = jnp.zeros((CODES, size), F32)
    for h in range(heads):
        summed = jnp.sum(table_parts[h], axis=1, keepdims=True)
        partial_table = jnp.where(lane128 == h, summed, partial_table)
    tgsend[...] = partial_table
    go(remote(tgsend, tgcore, core_s.at[4], core_r.at[4], partner))

    for off in range(1, NZ):
        zs = mod(z - off, NZ)
        for l in range(5):
            bit = bit_of(zs, l) if l < 3 else level_bits[l]
            arrived(zrecv_b.at[zs, l], zb_r.at[off, l], bit == 1)
    for l in range(2):
        @pl.when(level_bits[3 + l] == 1)
        def _(l=l):
            ring = zrecv_b[0, 3 + l].astype(F32)
            for zs in range(1, NZ):
                ring = ring + zrecv_b[zs, 3 + l].astype(F32)
            xsend_b[l] = ring.astype(BF16)
    for off in range(1, NX):
        xt = mod(x + off, NX)
        bit = jnp.where(lax.div(x, 2) == lax.div(xt, 2), 0, 1)
        go(remote(xsend_b.at[bit], xrecv_b.at[x], xb_s.at[off], xb_r.at[off], at_x(xt)), xt < x)

    weight_chip(1, x_left)
    weight_chip(2, x_right)
    arrived(wrelay.at[0], wx_r.at[0])
    wpart[x_left, c, top] = (wpart[x_left, c, top].astype(F32) + wrelay[0].astype(F32)).astype(BF16)
    go(remote(wpart.at[x_left, c], wxrecv.at[0], wx_s.at[2], wx_r.at[2], at_x(x_left)))
    arrived(wrelay.at[1], wx_r.at[1])
    wpart[x_right, c, low] = (wpart[x_right, c, low].astype(F32) + wrelay[1].astype(F32)).astype(BF16)
    go(remote(wpart.at[x_right, c], wxrecv.at[1], wx_s.at[3], wx_r.at[3], at_x(x_right)))

    arrived(tgcore, core_r.at[4])
    tgzsend[...] = tgsend[...] + tgcore[...]
    for off in range(1, NZ):
        go(remote(tgzsend, tgz.at[z], tz_s.at[off], tz_r.at[off], at_z(mod(z + off, NZ))))
    tgz[z] = tgzsend[...]

    for off in range(1, NX):
        xs = mod(x - off, NX)
        arrived(xrecv_b.at[xs], xb_r.at[off], xs > x)
    from_x = jnp.zeros((32, size), F32)
    for xs in range(1, NX):
        from_x = from_x + jnp.where(x < xs, xrecv_b[xs].astype(F32), 0.0)
    quad = zrecv_b[4, 2].astype(F32)
    for zs in range(5, NZ):
        quad = quad + zrecv_b[zs, 2].astype(F32)
    for zt in range(NZ):
        total = from_x
        if zt & 1 == 0:
            total = total + zrecv_b[zt + 1, 0].astype(F32)
        if zt & 2 == 0:
            upper = (zt // 4) * 4 + 2
            total = total + zrecv_b[upper, 1].astype(F32) + zrecv_b[upper + 1, 1].astype(F32)
        if zt & 4 == 0:
            total = total + quad
        gsend[zt] = total.astype(BF16)
    for off in range(1, NZ):
        zt = mod(z + off, NZ)
        go(remote(gsend.at[zt], gall.at[c, own_slice], rb_s.at[off], rb_r.at[off], at_z(zt)))
    gall[c, own_slice, :] = gsend[z]

    weight_chip(3, x)

    for off in range(1, NZ):
        zs = mod(z - off, NZ)
        arrived(gall.at[c, pl.ds(pl.multiple_of(zs * 32, 32), 32)], rb_r.at[off])
    go(remote(gall.at[c], gall.at[c], core_s.at[5], core_r.at[5], partner))

    arrived(wxrecv.at[0], wx_r.at[2])
    arrived(wxrecv.at[1], wx_r.at[3])
    wz[...] = (
        wpart[x, c].astype(F32) + wxrecv[0].astype(F32) + wxrecv[1].astype(F32)
    ).astype(BF16)
    for off in range(1, NZ):
        zt = mod(z + off, NZ)
        go(remote(wz.at[pl.ds(pl.multiple_of(zt * 32, 32), 32)], wzrecv.at[z],
                  wz_s.at[off], wz_r.at[off], at_z(zt)))
    wzrecv[z] = wz[own_slice, :]

    for off in range(1, NZ):
        arrived(tgz.at[mod(z - off, NZ)], tz_r.at[off])
    ring_table = tgz[0]
    for zs in range(1, NZ):
        ring_table = ring_table + tgz[zs]
    tgxsend[...] = ring_table
    for off in range(1, NX):
        go(remote(tgxsend, tgx.at[x], tx_s.at[off], tx_r.at[off], at_x(mod(x + off, NX))))
    tgx[x] = ring_table

    arrived(gall.at[other], core_r.at[5])
    arrived(t0recv, core_r.at[2])
    for h in range(heads):
        back = gall[h // 2, col(h % 2), :].astype(F32) + jnp.where(c == 0, t0recv[col(h), :].astype(F32), 0.0)
        back = back.astype(BF16)
        kg_ref[:, col(h)] = (kgl[:, col(h)] + mm(v_ref[:, col(h)], back, NT)).astype(BF16)
        vg_ref[:, col(h)] = (vgl[:, col(h)] + mm(k_ref[:, col(h)], back, NN)).astype(BF16)

    arrived(mrecv.at[0], m_r.at[2])
    arrived(mrecv.at[1], m_r.at[3])
    mixed_ref[...] = (
        mpart[y].astype(F32) + mrecv[0].astype(F32) + mrecv[1].astype(F32)
    ).astype(BF16)

    for off in range(1, NX):
        arrived(tgx.at[mod(x - off, NX)], tx_r.at[off])
    table = tgx[0]
    for xs in range(1, NX):
        table = table + tgx[xs]
    tokens = rows * 2 * NZ * NX
    square = jnp.concatenate([table, jnp.zeros((size - CODES, size), F32)], axis=0)
    tg_ref[...] = square.T[:heads, :CODES] * (1.0 / math.sqrt(tokens * levels))

    for off in range(1, NZ):
        arrived(wzrecv.at[mod(z - off, NZ)], wz_r.at[off])
    weight = wzrecv[0].astype(F32)
    for zs in range(1, NZ):
        weight = weight + wzrecv[zs].astype(F32)
    wg_ref[...] = weight * (1.0 / math.sqrt(tokens))

    for copy, cond in pending:
        if cond is None:
            copy.wait_send()
        else:
            pl.when(cond)(lambda copy=copy: copy.wait_send())


def store(*refs):
    sources, targets, sems = refs[:6], refs[6:12], refs[12]
    copies = [
        pltpu.make_async_copy(source, target, sems.at[i])
        for i, (source, target) in enumerate(zip(sources, targets))
    ]
    for copy in copies:
        copy.start()
    for copy in copies:
        copy.wait()


def per_device(queries, keys, values, level_table, level_code, out_weight, cotangent):
    rows, width = queries.shape
    vmem = pl.BlockSpec(memory_space=pltpu.VMEM)
    hbm = pl.BlockSpec(memory_space=pltpu.MemorySpace.HBM)
    smem = pl.BlockSpec(memory_space=pltpu.SMEM)
    dma = pltpu.SemaphoreType.DMA

    def bf(*shape):
        return pltpu.VMEM(shape, BF16)

    def f32(*shape):
        return pltpu.VMEM(shape, F32)

    scratch = [
        bf(rows, 512), bf(rows, 512), bf(rows, 512), bf(512, 2048), dma((5,)), bf(4, rows, 512), f32(4, 6, rows, 128), f32(4, rows, rows), f32(4, rows, rows),
        bf(4, rows, rows), bf(4, rows, 768), bf(rows, 512), bf(rows, 512),
        f32(rows, 512), f32(rows, 512), f32(rows, 512), f32(rows, 512),
        bf(512, 128), bf(512, 128), bf(256, 128), bf(NZ, 32, 128), bf(32, 128), bf(NX, 32, 128),
        bf(NZ, 3, 32, 128), bf(2, 32, 128), bf(5, 2, 256, 128),
        bf(512, 128), bf(512, 128), bf(5, 2, 256, 128), bf(5, 256, 128), bf(5, 256, 128),
        bf(NZ, 5, 32, 128), bf(2, 32, 128), bf(NX, 32, 128), bf(NZ, 32, 128), bf(2, 256, 128),
        bf(4, rows, 512), bf(2, rows // 2, 512), bf(2, rows, 512),
        bf(4, 2, 256, 512), bf(4, 256, 512), bf(2, 128, 512), bf(2, 256, 512), bf(256, 512),
        bf(NZ, 32, 512),
        f32(CODES, 128), f32(CODES, 128), f32(CODES, 128), f32(NZ, CODES, 128),
        f32(CODES, 128), f32(NX, CODES, 128),
        dma((6,)), dma((6,)), dma((6,)), dma((6,)), dma((NZ,)), dma((NZ,)), dma((NX,)), dma((NX,)),
        dma((NZ, 5)), dma((NZ, 5)), dma((NZ, 5)), dma((NZ, 5)), dma((NX,)), dma((NX,)),
        dma((NZ,)), dma((NZ,)), dma((4,)), dma((4,)), dma((4,)), dma((4,)), dma((4,)), dma((4,)),
        dma((NZ,)), dma((NZ,)), dma((NZ,)), dma((NZ,)), dma((NX,)), dma((NX,)),
    ]
    shape = jax.ShapeDtypeStruct
    results = pl.pallas_call(
        kernel,
        out_shape=(
            shape((rows, width), BF16),
            shape((32, width), F32),
            shape((rows, width), BF16),
            shape((rows, width), BF16),
            shape((rows, width), BF16),
            shape((4, CODES), F32),
        ),
        in_specs=[hbm, hbm, hbm, smem, vmem, hbm, hbm],
        out_specs=[vmem] * 6,
        scratch_shapes=scratch,
        compiler_params=pltpu.CompilerParams(
            collective_id=0, has_side_effects=True, vmem_limit_bytes=53900 * 2**10
        ),
        name="layer",
    )(queries, keys, values, level_table.T, level_code.T, out_weight, cotangent)
    stored = pl.pallas_call(
        store,
        out_shape=tuple(shape(value.shape, value.dtype) for value in results),
        in_specs=[vmem] * 6,
        out_specs=[pl.BlockSpec(memory_space=pl.ANY)] * 6,
        scratch_shapes=[dma((6,))],
        compiler_params=pltpu.CompilerParams(vmem_limit_bytes=2**20),
        name="store",
    )(*results)
    return (*stored[:5], stored[5].T)


def solution(mesh):
    wide = P("seq", "head")
    return jax.shard_map(
        per_device,
        mesh=mesh,
        in_specs=(wide, wide, wide, P(None, "head"), P("seq", None), P("head", None), wide),
        out_specs=(wide, wide, wide, wide, wide, P(None, "head")),
        check_vma=False,
    )
```

```python
import math

import jax
import jax.numpy as jnp
from jax import lax
from jax.experimental import pallas as pl
from jax.experimental.pallas import tpu as pltpu
from jax.sharding import PartitionSpec as P

SPAN = 64
CODES = 16
NX, NZ = 4, 8
F32, BF16 = jnp.float32, jnp.bfloat16
MESH = pl.DeviceIdType.MESH
NN = (((1,), (0,)), ((), ()))
NT = (((1,), (1,)), ((), ()))
TN = (((0,), (0,)), ((), ()))


def mm(left, right, dims):
    return lax.dot_general(left, right, dims, preferred_element_type=F32)


def remote(src, dst, send_sem, recv_sem, device):
    return pltpu.make_async_remote_copy(
        src_ref=src,
        dst_ref=dst,
        send_sem=send_sem,
        recv_sem=recv_sem,
        device_id=device,
        device_id_type=MESH,
    )


def mod(value, size):
    return lax.rem(value + size, size)


def bit_of(value, index):
    return lax.rem(lax.div(value, 2**index), 2)


def kernel(
    q_hbm, k_hbm, v_hbm, table_ref, code_ref, w_hbm, cot_hbm,
    mixed_ref, wg_ref, qg_ref, kg_ref, vg_ref, tg_ref,
    q_ref, k_ref, v_ref, w_ref, load_sems, far_sems, reads, cotall, coefb, scores, lw, probs, sgbuf, gbuf, abuf, attnl, qgl, kgl, vgl,
    dsend, drecv, zsend_f, zrecv_f, xsend_f, xrecv_f, rsend_f, rx_f, fall,
    t0send, t0recv, tsend, trecv, zsend_b, zrecv_b, xsend_b, xrecv_b, gsend, gall,
    mpart, mrelay, mrecv, wpart, wrecv, wrelay, wxrecv, wz, wzrecv,
    tgsend, tgcore, tgzsend, tgz, tgxsend, tgx,
    cot_s, cot_r, core_s, core_r, zf_s, zf_r, xf_s, xf_r, rf_s, rf_r,
    zb_s, zb_r, xb_s, xb_r, rb_s, rb_r, m_s, m_r, wc_s, wc_r, wx_s, wx_r, wz_s, wz_r,
    tz_s, tz_r, tx_s, tx_r,
):
    s = lax.axis_index("seq")
    y = lax.axis_index("head")
    c = lax.rem(s, 2)
    z = lax.rem(lax.div(s, 2), NZ)
    x = lax.div(s, 2 * NZ)
    other = 1 - c
    heads, size = 4, 128
    rows = q_ref.shape[0]
    loads = [
        pltpu.make_async_copy(source, target, load_sems.at[i])
        for i, (source, target) in enumerate(
            [(cot_hbm, cotall.at[y]), (k_hbm, k_ref), (v_hbm, v_ref), (q_hbm, q_ref), (w_hbm, w_ref)]
        )
    ]
    for load in loads:
        load.start()
    half = rows // 2

    def at_y(target):
        return (s, target)

    def at_z(target):
        return ((x * NZ + target) * 2 + c, y)

    def at_x(target):
        return ((target * NZ + z) * 2 + c, y)

    partner = (s + 1 - 2 * c, y)
    level_bits = [bit_of(z, 0), bit_of(z, 1), bit_of(z, 2), bit_of(x, 0), bit_of(x, 1)]
    pending = []

    def go(copy, cond=None):
        pending.append((copy, cond))
        if cond is None:
            copy.start()
        else:
            pl.when(cond)(lambda: copy.start())

    def arrived(dst, sem, cond=None):
        copy = remote(dst, dst, sem, sem, partner)
        if cond is None:
            copy.wait_recv()
        else:
            pl.when(cond)(lambda: copy.wait_recv())

    def col(h):
        return slice(h * size, (h + 1) * size)

    right, left = mod(y + 1, 4), mod(y - 1, 4)
    x_right, x_left, x_opposite = mod(x + 1, 4), mod(x - 1, 4), mod(x + 2, 4)
    z_next, z_last = mod(z + 1, NZ), mod(z - 1, NZ)
    barrier = pltpu.get_barrier_semaphore()
    near = [partner, at_y(right), at_y(left), at_z(z_next), at_z(z_last), at_x(x_right), at_x(x_left)]
    for device in near:
        pl.semaphore_signal(barrier, inc=1, device_id=device, device_id_type=MESH)

    def tell(index, device):
        pl.semaphore_signal(far_sems.at[index], inc=1, device_id=device, device_id_type=MESH)

    def tell_z():
        tell(0, at_z(z_next))
        tell(1, at_z(z_last))

    def hear_z():
        pl.semaphore_wait(far_sems.at[0], 1)
        pl.semaphore_wait(far_sems.at[1], 1)

    loads[1].wait()
    loads[2].wait()
    for h in range(heads):
        dsend[col(h), :] = mm(k_ref[:, col(h)], v_ref[:, col(h)], TN).astype(BF16)
    for l in range(5):
        @pl.when(level_bits[l] == 0)
        def _(l=l):
            fall[l, c] = jnp.zeros((256, size), BF16)
    loads[0].wait()
    pl.semaphore_wait(barrier, len(near))

    top, low = pl.ds(0, half), pl.ds(half, half)
    go(remote(cotall.at[y, top], cotall.at[y, top], cot_s.at[0], cot_r.at[0], at_y(right)))
    go(remote(cotall.at[y, low], cotall.at[y, low], cot_s.at[2], cot_r.at[2], at_y(left)))
    go(remote(cotall.at[y, low], cotall.at[y, low], cot_s.at[1], cot_r.at[1], at_y(right)))
    go(remote(cotall.at[y, top], cotall.at[y, top], cot_s.at[3], cot_r.at[3], at_y(left)))
    go(remote(dsend, drecv, core_s.at[0], core_r.at[0], partner))
    tell(2, at_x(x_right))
    tell(3, at_x(x_left))
    tell_z()

    levels = code_ref.shape[0]
    code_t = code_ref[...].astype(F32)
    padding = jnp.zeros((size - levels, rows), F32)
    code = jnp.concatenate([code_t, padding], axis=0).T
    lane = lax.broadcasted_iota(jnp.int32, (1, size), 1)
    scale = jnp.zeros((1, size), F32)
    scales = [1.0 / math.sqrt(SPAN * 2 ** max(l - 1, 0)) for l in range(levels)]
    for l in range(levels):
        scale = jnp.where(lane == l, scales[l], scale)
    coefs = []
    for h in range(heads):
        lam = jnp.zeros((rows, size), F32)
        for entry in range(CODES):
            lam = jnp.where(code == float(entry), table_ref[h:h + 1, entry:entry + 1], lam)
        coefs.append(lam * scale)

    pl.semaphore_wait(far_sems.at[2], 1)
    pl.semaphore_wait(far_sems.at[3], 1)
    hear_z()
    tell_z()

    loads[3].wait()
    row = lax.broadcasted_iota(jnp.int32, (rows, rows), 0)
    column = lax.broadcasted_iota(jnp.int32, (rows, rows), 1)
    row_span, column_span = row // SPAN, column // SPAN
    in_level = [
        (row_span == column_span) & (column <= row),
        (row_span // 2 == column_span // 2) & (column_span < row_span),
        (row_span >= 2) & (column_span < 2),
    ]

    def local_forward(h):
        weight = jnp.zeros((rows, rows), F32)
        for l in range(3):
            weight = jnp.where(in_level[l], coefs[h][:, l:l + 1], weight)
        score = mm(q_ref[:, col(h)], k_ref[:, col(h)], NT)
        scores[h] = score
        lw[h] = weight
        prob = (score * weight).astype(BF16)
        probs[h] = prob
        attnl[:, col(h)] = mm(prob, v_ref[:, col(h)], NN)

    for h in range(2):
        local_forward(h)
    hear_z()
    tell_z()
    arrived(drecv, core_r.at[0])
    half_rows = pl.ds(pl.multiple_of(c * 256, 256), 256)
    zsend_f[...] = (dsend[half_rows, :].astype(F32) + drecv[half_rows, :].astype(F32)).astype(BF16)
    hear_z()
    for off in range(1, NZ):
        zt = mod(z + off, NZ)
        go(remote(zsend_f.at[pl.ds(pl.multiple_of(zt * 32, 32), 32)], zrecv_f.at[z],
                  zf_s.at[off], zf_r.at[off], at_z(zt)))
    own_slice = pl.ds(pl.multiple_of(z * 32, 32), 32)
    zrecv_f[z] = zsend_f[own_slice, :]

    for h in range(2, heads):
        local_forward(h)
    for h in range(heads):
        for l in range(3, levels):
            coefb[h, l - 3] = jnp.broadcast_to(coefs[h][:, l:l + 1], (rows, size))

    arrived(cotall.at[left, top], cot_r.at[0])
    go(remote(cotall.at[left, top], cotall.at[left, top], cot_s.at[4], cot_r.at[4], at_y(right)))
    arrived(cotall.at[right, low], cot_r.at[2])
    go(remote(cotall.at[right, low], cotall.at[right, low], cot_s.at[5], cot_r.at[5], at_y(left)))

    for off in range(1, NZ):
        arrived(zrecv_f.at[mod(z - off, NZ)], zf_r.at[off])
    parts = [zrecv_f[i].astype(F32) for i in range(NZ)]
    pairs = [parts[2 * i] + parts[2 * i + 1] for i in range(4)]
    quads = [pairs[0] + pairs[1], pairs[2] + pairs[3]]
    xsend_f[...] = (quads[0] + quads[1]).astype(BF16)
    for off in range(1, NX):
        xt = mod(x + off, NX)
        go(remote(xsend_f, xrecv_f.at[x], xf_s.at[off], xf_r.at[off], at_x(xt)), xt > x)
    for zt in range(NZ):
        if zt & 1:
            rsend_f[zt, 0] = parts[zt - 1].astype(BF16)
        if zt & 2:
            rsend_f[zt, 1] = pairs[2 * (zt // 4)].astype(BF16)
        if zt & 4:
            rsend_f[zt, 2] = quads[0].astype(BF16)
    for off in range(1, NZ):
        zt = mod(z + off, NZ)
        for l in range(3):
            go(remote(rsend_f.at[zt, l], fall.at[l, c, own_slice],
                      rf_s.at[off, l], rf_r.at[off, l], at_z(zt)), bit_of(zt, l) == 1)
    for l in range(3):
        @pl.when(level_bits[l] == 1)
        def _(l=l):
            fall[l, c, own_slice, :] = rsend_f[z, l]

    for off in range(1, NX):
        xs = mod(x - off, NX)
        arrived(xrecv_f.at[xs], xf_r.at[off], xs < x)

    @pl.when(bit_of(x, 0) == 1)
    def _():
        rx_f[0] = xrecv_f[x - 1]
        fall[3, c, own_slice, :] = xrecv_f[x - 1]

    @pl.when(x >= 2)
    def _():
        both = (xrecv_f[0].astype(F32) + xrecv_f[1].astype(F32)).astype(BF16)
        rx_f[1] = both
        fall[4, c, own_slice, :] = both

    for off in range(1, NZ):
        zt = mod(z + off, NZ)
        for l in range(3, 5):
            go(remote(rx_f.at[l - 3], fall.at[l, c, own_slice],
                      rf_s.at[off, l], rf_r.at[off, l], at_z(zt)), level_bits[l] == 1)

    loads[4].wait()
    opposite = mod(y + 2, 4)
    arrived(cotall.at[left, low], cot_r.at[1])
    arrived(cotall.at[right, top], cot_r.at[3])
    arrived(cotall.at[opposite, top], cot_r.at[4])
    arrived(cotall.at[opposite, low], cot_r.at[5])
    full_rows = jnp.concatenate([cotall[i] for i in range(4)], axis=1)
    gbuf[...] = mm(full_rows, w_ref[...], NT).astype(BF16)

    for h in range(heads):
        grad = gbuf[:, col(h)].astype(F32)
        for l in range(6):
            sgbuf[h, :, col(l)] = (coefb[h, l] * grad).astype(BF16)
        terms = mm(q_ref[:, col(h)], sgbuf[h], TN)
        t0send[col(h), :] = terms[:, col(0)].astype(BF16)
        for l in range(5):
            tsend[l, h // 2, col(h % 2), :] = terms[:, col(l + 1)].astype(BF16)
    go(remote(tsend.at[:, other], trecv, core_s.at[1], core_r.at[1], partner))
    go(remote(t0send, t0recv, core_s.at[2], core_r.at[2], partner))

    for off in range(1, NZ):
        zs = mod(z - off, NZ)
        zs_slice = pl.ds(pl.multiple_of(zs * 32, 32), 32)
        for l in range(5):
            arrived(fall.at[l, c, zs_slice], rf_r.at[off, l], level_bits[l] == 1)
    go(remote(fall.at[:, c], fall.at[:, c], core_s.at[3], core_r.at[3], partner))

    arrived(trecv, core_r.at[1])
    for l in range(5):
        zsend_b[l] = (tsend[l, c].astype(F32) + trecv[l].astype(F32)).astype(BF16)
    for off in range(1, NZ):
        zt = mod(z + off, NZ)
        for l in range(5):
            go(remote(zsend_b.at[l, pl.ds(pl.multiple_of(zt * 32, 32), 32)], zrecv_b.at[z, l],
                      zb_s.at[off, l], zb_r.at[off, l], at_z(zt)), level_bits[l] == 1)
    for l in range(5):
        @pl.when(level_bits[l] == 1)
        def _(l=l):
            zrecv_b[z, l] = zsend_b[l, own_slice, :]

    arrived(fall.at[:, other], core_r.at[3])

    def found_states(h):
        found = [jnp.where(c == 1, drecv[col(h), :], jnp.zeros((size, size), BF16))]
        found += [fall[l, h // 2, col(h % 2), :] for l in range(5)]
        return jnp.concatenate(found, axis=1)

    for h in range(heads):
        values = mm(q_ref[:, col(h)], found_states(h), NN)
        reads[h] = values
        attention = attnl[:, col(h)]
        for l in range(6):
            attention = attention + coefb[h, l] * values[:, col(l)]
        abuf[:, col(h)] = attention.astype(BF16)

    def weight_part(step, target):
        part = mm(cotall[target], abuf[...], TN)
        for block in range(16):
            wpart[target, block % 2, pl.ds((block // 2) * 32, 32), :] = (
                part[block * 32:(block + 1) * 32].astype(BF16)
            )
        go(remote(wpart.at[target, other], wrecv.at[target], wc_s.at[step], wc_r.at[step], partner))

    def weight_chip(step, target):
        arrived(wrecv.at[target], wc_r.at[step])
        wpart[target, c] = (wpart[target, c].astype(F32) + wrecv[target].astype(F32)).astype(BF16)

    def product_for(target):
        columns = pl.ds(pl.multiple_of(target * 512, 512), 512)
        mpart[target] = mm(abuf[...], w_ref[:, columns], NN).astype(BF16)

    sides = [pl.ds(0, 256), pl.ds(256, 256)]
    weight_part(0, x_opposite)
    product_for(opposite)
    go(remote(mpart.at[opposite, top], mrelay.at[0], m_s.at[0], m_r.at[0], at_y(left)))
    go(remote(mpart.at[opposite, low], mrelay.at[1], m_s.at[1], m_r.at[1], at_y(right)))
    weight_part(1, x_left)
    weight_chip(0, x_opposite)
    for i in range(2):
        go(remote(wpart.at[x_opposite, c, top, sides[i]], wrelay.at[0, :, sides[i]],
                  wx_s.at[4 * i], wx_r.at[4 * i], at_x(x_left)))
        go(remote(wpart.at[x_opposite, c, low, sides[i]], wrelay.at[1, :, sides[i]],
                  wx_s.at[4 * i + 1], wx_r.at[4 * i + 1], at_x(x_right)))
    weight_part(2, x_right)
    product_for(left)
    product_for(right)
    weight_chip(1, x_left)
    weight_chip(2, x_right)

    entry_row = lax.broadcasted_iota(jnp.int32, (CODES, rows), 0).astype(F32)
    one_hot = [
        jnp.where(jnp.broadcast_to(code_t[l:l + 1, :], (CODES, rows)) == entry_row, 1.0, 0.0).astype(BF16)
        for l in range(levels)
    ]
    table_parts = []

    def local_back(h):
        grad = gbuf[:, col(h)]
        prob_grad = mm(grad, v_ref[:, col(h)], NT)
        score_grad = (prob_grad * lw[h]).astype(BF16)
        product = scores[h] * prob_grad
        total = jnp.zeros((CODES, rows), F32)
        for l in range(3):
            masked = jnp.where(in_level[l], product, 0.0).astype(BF16)
            total = total + scales[l] * mm(one_hot[l], masked, NN)
        qgl[:, col(h)] = mm(score_grad, k_ref[:, col(h)], NN)
        kgl[:, col(h)] = mm(score_grad, q_ref[:, col(h)], TN)
        vgl[:, col(h)] = mm(probs[h], grad, TN)
        table_parts.append(total[:, :size] + total[:, size:])

    for h in range(heads):
        local_back(h)

    for off in range(1, NZ):
        zs = mod(z - off, NZ)
        for l in range(5):
            bit = bit_of(zs, l) if l < 3 else level_bits[l]
            arrived(zrecv_b.at[zs, l], zb_r.at[off, l], bit == 1)
    for l in range(2):
        @pl.when(level_bits[3 + l] == 1)
        def _(l=l):
            ring = zrecv_b[0, 3 + l].astype(F32)
            for zs in range(1, NZ):
                ring = ring + zrecv_b[zs, 3 + l].astype(F32)
            xsend_b[l] = ring.astype(BF16)
    for off in range(1, NX):
        xt = mod(x + off, NX)
        bit = jnp.where(lax.div(x, 2) == lax.div(xt, 2), 0, 1)
        go(remote(xsend_b.at[bit], xrecv_b.at[x], xb_s.at[off], xb_r.at[off], at_x(xt)), xt < x)

    def weight_relay(i):
        side = sides[i]
        arrived(wrelay.at[0, :, side], wx_r.at[4 * i])
        wpart[x_left, c, top, side] = (
            wpart[x_left, c, top, side].astype(F32) + wrelay[0, :, side].astype(F32)
        ).astype(BF16)
        go(remote(wpart.at[x_left, c, :, side], wxrecv.at[0, :, side],
                  wx_s.at[4 * i + 2], wx_r.at[4 * i + 2], at_x(x_left)))
        arrived(wrelay.at[1, :, side], wx_r.at[4 * i + 1])
        wpart[x_right, c, low, side] = (
            wpart[x_right, c, low, side].astype(F32) + wrelay[1, :, side].astype(F32)
        ).astype(BF16)
        go(remote(wpart.at[x_right, c, :, side], wxrecv.at[1, :, side],
                  wx_s.at[4 * i + 3], wx_r.at[4 * i + 3], at_x(x_right)))

    weight_relay(0)
    weight_part(3, x)
    product_for(y)
    weight_relay(1)

    for off in range(1, NX):
        xs = mod(x - off, NX)
        arrived(xrecv_b.at[xs], xb_r.at[off], xs > x)
    from_x = jnp.zeros((32, size), F32)
    for xs in range(1, NX):
        from_x = from_x + jnp.where(x < xs, xrecv_b[xs].astype(F32), 0.0)
    quad = zrecv_b[4, 2].astype(F32)
    for zs in range(5, NZ):
        quad = quad + zrecv_b[zs, 2].astype(F32)
    for zt in range(NZ):
        total = from_x
        if zt & 1 == 0:
            total = total + zrecv_b[zt + 1, 0].astype(F32)
        if zt & 2 == 0:
            upper = (zt // 4) * 4 + 2
            total = total + zrecv_b[upper, 1].astype(F32) + zrecv_b[upper + 1, 1].astype(F32)
        if zt & 4 == 0:
            total = total + quad
        gsend[zt] = total.astype(BF16)
    for off in range(1, NZ):
        zt = mod(z + off, NZ)
        go(remote(gsend.at[zt], gall.at[c, own_slice], rb_s.at[off], rb_r.at[off], at_z(zt)))
    gall[c, own_slice, :] = gsend[z]

    arrived(mrelay.at[0], m_r.at[0])
    mpart[left, top] = (mpart[left, top].astype(F32) + mrelay[0].astype(F32)).astype(BF16)
    go(remote(mpart.at[left], mrecv.at[0], m_s.at[2], m_r.at[2], at_y(left)))
    arrived(mrelay.at[1], m_r.at[1])
    mpart[right, low] = (mpart[right, low].astype(F32) + mrelay[1].astype(F32)).astype(BF16)
    go(remote(mpart.at[right], mrecv.at[1], m_s.at[3], m_r.at[3], at_y(right)))

    for h in range(heads):
        grad = gbuf[:, col(h)].astype(F32)
        total = table_parts[h]
        for l in range(6):
            total = total + scales[l + 3] * mm(one_hot[l + 3], (grad * reads[h, :, col(l)]).astype(BF16), NN)
        table_parts[h] = total
        qg_ref[:, col(h)] = (qgl[:, col(h)] + mm(sgbuf[h], found_states(h), NT)).astype(BF16)
    lane128 = lax.broadcasted_iota(jnp.int32, (CODES, size), 1)
    partial_table = jnp.zeros((CODES, size), F32)
    for h in range(heads):
        summed = jnp.sum(table_parts[h], axis=1, keepdims=True)
        partial_table = jnp.where(lane128 == h, summed, partial_table)
    tgsend[...] = partial_table
    go(remote(tgsend, tgcore, core_s.at[4], core_r.at[4], partner))

    arrived(tgcore, core_r.at[4])
    tgzsend[...] = tgsend[...] + tgcore[...]
    for off in range(1, NZ):
        go(remote(tgzsend, tgz.at[z], tz_s.at[off], tz_r.at[off], at_z(mod(z + off, NZ))))
    tgz[z] = tgzsend[...]
    weight_chip(3, x)

    def weight_ring(i):
        side = sides[i]
        arrived(wxrecv.at[0, :, side], wx_r.at[4 * i + 2])
        arrived(wxrecv.at[1, :, side], wx_r.at[4 * i + 3])
        wz[:, side] = (
            wpart[x, c, :, side].astype(F32) + wxrecv[0, :, side].astype(F32) + wxrecv[1, :, side].astype(F32)
        ).astype(BF16)
        for off in range(1, NZ):
            zt = mod(z + off, NZ)
            go(remote(wz.at[pl.ds(pl.multiple_of(zt * 32, 32), 32), side], wzrecv.at[z, :, side],
                      wz_s.at[off, i], wz_r.at[off, i], at_z(zt)))
        wzrecv[z, :, side] = wz[own_slice, side]

    weight_ring(0)
    for off in range(1, NZ):
        zs = mod(z - off, NZ)
        arrived(gall.at[c, pl.ds(pl.multiple_of(zs * 32, 32), 32)], rb_r.at[off])
    go(remote(gall.at[c], gall.at[c], core_s.at[5], core_r.at[5], partner))
    weight_ring(1)

    for off in range(1, NZ):
        arrived(tgz.at[mod(z - off, NZ)], tz_r.at[off])
    ring_table = tgz[0]
    for zs in range(1, NZ):
        ring_table = ring_table + tgz[zs]
    tgxsend[...] = ring_table
    for off in range(1, NX):
        go(remote(tgxsend, tgx.at[x], tx_s.at[off], tx_r.at[off], at_x(mod(x + off, NX))))
    tgx[x] = ring_table

    arrived(gall.at[other], core_r.at[5])
    arrived(t0recv, core_r.at[2])
    for h in range(heads):
        back = gall[h // 2, col(h % 2), :].astype(F32) + jnp.where(c == 0, t0recv[col(h), :].astype(F32), 0.0)
        back = back.astype(BF16)
        kg_ref[:, col(h)] = (kgl[:, col(h)] + mm(v_ref[:, col(h)], back, NT)).astype(BF16)
        vg_ref[:, col(h)] = (vgl[:, col(h)] + mm(k_ref[:, col(h)], back, NN)).astype(BF16)

    arrived(mrecv.at[0], m_r.at[2])
    arrived(mrecv.at[1], m_r.at[3])
    mixed_ref[...] = (
        mpart[y].astype(F32) + mrecv[0].astype(F32) + mrecv[1].astype(F32)
    ).astype(BF16)

    for off in range(1, NX):
        arrived(tgx.at[mod(x - off, NX)], tx_r.at[off])
    table = tgx[0]
    for xs in range(1, NX):
        table = table + tgx[xs]
    tokens = rows * 2 * NZ * NX
    square = jnp.concatenate([table, jnp.zeros((size - CODES, size), F32)], axis=0)
    tg_ref[...] = square.T[:heads, :CODES] * (1.0 / math.sqrt(tokens * levels))

    for i in range(2):
        for off in range(1, NZ):
            arrived(wzrecv.at[mod(z - off, NZ), :, sides[i]], wz_r.at[off, i])
        weight = wzrecv[0, :, sides[i]].astype(F32)
        for zs in range(1, NZ):
            weight = weight + wzrecv[zs, :, sides[i]].astype(F32)
        wg_ref[:, sides[i]] = weight * (1.0 / math.sqrt(tokens))

    for copy, cond in pending:
        if cond is None:
            copy.wait_send()
        else:
            pl.when(cond)(lambda copy=copy: copy.wait_send())


def store(*refs):
    sources, targets, sems = refs[:6], refs[6:12], refs[12]
    copies = [
        pltpu.make_async_copy(source, target, sems.at[i])
        for i, (source, target) in enumerate(zip(sources, targets))
    ]
    for copy in copies:
        copy.start()
    for copy in copies:
        copy.wait()


def per_device(queries, keys, values, level_table, level_code, out_weight, cotangent):
    rows, width = queries.shape
    vmem = pl.BlockSpec(memory_space=pltpu.VMEM)
    hbm = pl.BlockSpec(memory_space=pltpu.MemorySpace.HBM)
    dma = pltpu.SemaphoreType.DMA

    def bf(*shape):
        return pltpu.VMEM(shape, BF16)

    def f32(*shape):
        return pltpu.VMEM(shape, F32)

    scratch = [
        bf(rows, 512), bf(rows, 512), bf(rows, 512), bf(512, 2048), dma((5,)),
        pltpu.SemaphoreType.REGULAR((4,)), f32(4, rows, 768), bf(4, rows, 512), f32(4, 6, rows, 128), f32(4, rows, rows), f32(4, rows, rows),
        bf(4, rows, rows), bf(4, rows, 768), bf(rows, 512), bf(rows, 512),
        f32(rows, 512), f32(rows, 512), f32(rows, 512), f32(rows, 512),
        bf(512, 128), bf(512, 128), bf(256, 128), bf(NZ, 32, 128), bf(32, 128), bf(NX, 32, 128),
        bf(NZ, 3, 32, 128), bf(2, 32, 128), bf(5, 2, 256, 128),
        bf(512, 128), bf(512, 128), bf(5, 2, 256, 128), bf(5, 256, 128), bf(5, 256, 128),
        bf(NZ, 5, 32, 128), bf(2, 32, 128), bf(NX, 32, 128), bf(NZ, 32, 128), bf(2, 256, 128),
        bf(4, rows, 512), bf(2, rows // 2, 512), bf(2, rows, 512),
        bf(4, 2, 256, 512), bf(4, 256, 512), bf(2, 128, 512), bf(2, 256, 512), bf(256, 512),
        bf(NZ, 32, 512),
        f32(CODES, 128), f32(CODES, 128), f32(CODES, 128), f32(NZ, CODES, 128),
        f32(CODES, 128), f32(NX, CODES, 128),
        dma((6,)), dma((6,)), dma((6,)), dma((6,)), dma((NZ,)), dma((NZ,)), dma((NX,)), dma((NX,)),
        dma((NZ, 5)), dma((NZ, 5)), dma((NZ, 5)), dma((NZ, 5)), dma((NX,)), dma((NX,)),
        dma((NZ,)), dma((NZ,)), dma((4,)), dma((4,)), dma((4,)), dma((4,)), dma((8,)), dma((8,)),
        dma((NZ, 2)), dma((NZ, 2)), dma((NZ,)), dma((NZ,)), dma((NX,)), dma((NX,)),
    ]
    shape = jax.ShapeDtypeStruct
    results = pl.pallas_call(
        kernel,
        out_shape=(
            shape((rows, width), BF16),
            shape((32, width), F32),
            shape((rows, width), BF16),
            shape((rows, width), BF16),
            shape((rows, width), BF16),
            shape((4, CODES), F32),
        ),
        in_specs=[hbm, hbm, hbm, vmem, vmem, hbm, hbm],
        out_specs=[vmem] * 6,
        scratch_shapes=scratch,
        compiler_params=pltpu.CompilerParams(
            collective_id=0, has_side_effects=True, vmem_limit_bytes=53900 * 2**10
        ),
        name="layer",
    )(queries, keys, values, level_table.T, level_code.T, out_weight, cotangent)
    stored = pl.pallas_call(
        store,
        out_shape=tuple(shape(value.shape, value.dtype) for value in results),
        in_specs=[vmem] * 6,
        out_specs=[pl.BlockSpec(memory_space=pl.ANY)] * 6,
        scratch_shapes=[dma((6,))],
        compiler_params=pltpu.CompilerParams(vmem_limit_bytes=2**20),
        name="store",
    )(*results)
    return (*stored[:5], stored[5].T)


def solution(mesh):
    wide = P("seq", "head")
    return jax.shard_map(
        per_device,
        mesh=mesh,
        in_specs=(wide, wide, wide, P(None, "head"), P("seq", None), P("head", None), wide),
        out_specs=(wide, wide, wide, wide, wide, P(None, "head")),
        check_vma=False,
    )
```

```python
import math

import jax
import jax.numpy as jnp
from jax import lax
from jax.experimental import pallas as pl
from jax.experimental.pallas import tpu as pltpu
from jax.sharding import PartitionSpec as P

SPAN = 64
CODES = 16
NX, NZ = 4, 8
Z_ORDER = (4, 3, 5, 2, 6, 1, 7)
PIECES = 4
F32, BF16 = jnp.float32, jnp.bfloat16
MESH = pl.DeviceIdType.MESH
NN = (((1,), (0,)), ((), ()))
NT = (((1,), (1,)), ((), ()))
TN = (((0,), (0,)), ((), ()))


def mm(left, right, dims):
    return lax.dot_general(left, right, dims, preferred_element_type=F32)


def remote(src, dst, send_sem, recv_sem, device):
    return pltpu.make_async_remote_copy(
        src_ref=src,
        dst_ref=dst,
        send_sem=send_sem,
        recv_sem=recv_sem,
        device_id=device,
        device_id_type=MESH,
    )


def mod(value, size):
    return lax.rem(value + size, size)


def bit_of(value, index):
    return lax.rem(lax.div(value, 2**index), 2)


def kernel(
    q_hbm, k_hbm, v_hbm, table_ref, code_ref, w_hbm, cot_hbm,
    mixed_ref, wg_ref, qg_ref, kg_ref, vg_ref, tg_ref,
    q_ref, k_ref, v_ref, w_ref, load_sems, far_sems, reads, cotall, coefb, scores, lw, probs, sgbuf, gbuf, abuf, attnl, qgl, kgl, vgl,
    dsend, drecv, zsend_f, zrecv_f, xsend_f, xrecv_f, rsend_f, rx_f, fall,
    t0send, t0recv, tsend, trecv, zsend_b, zrecv_b, xsend_b, xrecv_b, gsend, gall,
    mpart, mrelay, mrecv, wpart, wrecv, wrelay, wxrecv, wz, wzrecv,
    tgsend, tgcore, tgzsend, tgz, tgxsend, tgx,
    cot_s, cot_r, core_s, core_r, zf_s, zf_r, xf_s, xf_r, rf_s, rf_r,
    zb_s, zb_r, xb_s, xb_r, rb_s, rb_r, m_s, m_r, wc_s, wc_r, wx_s, wx_r, wz_s, wz_r,
    tz_s, tz_r, tx_s, tx_r,
):
    s = lax.axis_index("seq")
    y = lax.axis_index("head")
    c = lax.rem(s, 2)
    z = lax.rem(lax.div(s, 2), NZ)
    x = lax.div(s, 2 * NZ)
    other = 1 - c
    heads, size = 4, 128
    rows = q_ref.shape[0]
    loads = [
        pltpu.make_async_copy(source, target, load_sems.at[i])
        for i, (source, target) in enumerate(
            [(cot_hbm, cotall.at[y]), (k_hbm, k_ref), (v_hbm, v_ref), (q_hbm, q_ref), (w_hbm, w_ref)]
        )
    ]
    for load in loads:
        load.start()
    half = rows // 2

    def at_y(target):
        return (s, target)

    def at_z(target):
        return ((x * NZ + target) * 2 + c, y)

    def at_x(target):
        return ((target * NZ + z) * 2 + c, y)

    partner = (s + 1 - 2 * c, y)
    level_bits = [bit_of(z, 0), bit_of(z, 1), bit_of(z, 2), bit_of(x, 0), bit_of(x, 1)]
    pending = []

    def go(copy, cond=None):
        pending.append((copy, cond))
        if cond is None:
            copy.start()
        else:
            pl.when(cond)(lambda: copy.start())

    def arrived(dst, sem, cond=None):
        copy = remote(dst, dst, sem, sem, partner)
        if cond is None:
            copy.wait_recv()
        else:
            pl.when(cond)(lambda: copy.wait_recv())

    def col(h):
        return slice(h * size, (h + 1) * size)

    right, left = mod(y + 1, 4), mod(y - 1, 4)
    x_right, x_left, x_opposite = mod(x + 1, 4), mod(x - 1, 4), mod(x + 2, 4)
    barrier = pltpu.get_barrier_semaphore()
    near = [partner, at_y(right), at_y(left), at_x(x_right), at_x(x_left), at_x(x_opposite)]
    near += [at_z(mod(z + off, NZ)) for off in (1, -1, 2, -2)]
    for device in near:
        pl.semaphore_signal(barrier, inc=1, device_id=device, device_id_type=MESH)

    def tell(index, device):
        pl.semaphore_signal(far_sems.at[index], inc=1, device_id=device, device_id_type=MESH)

    def tell_z():
        tell(0, at_z(mod(z + 2, NZ)))
        tell(1, at_z(mod(z - 2, NZ)))

    def hear_z():
        pl.semaphore_wait(far_sems.at[0], 1)
        pl.semaphore_wait(far_sems.at[1], 1)

    loads[1].wait()
    loads[2].wait()
    for h in range(heads):
        dsend[col(h), :] = mm(k_ref[:, col(h)], v_ref[:, col(h)], TN).astype(BF16)
    for l in range(5):
        @pl.when(level_bits[l] == 0)
        def _(l=l):
            fall[l, c] = jnp.zeros((256, size), BF16)
    loads[0].wait()
    pl.semaphore_wait(barrier, len(near))

    top, low = pl.ds(0, half), pl.ds(half, half)
    go(remote(cotall.at[y, top], cotall.at[y, top], cot_s.at[0], cot_r.at[0], at_y(right)))
    go(remote(cotall.at[y, low], cotall.at[y, low], cot_s.at[2], cot_r.at[2], at_y(left)))
    go(remote(cotall.at[y, low], cotall.at[y, low], cot_s.at[1], cot_r.at[1], at_y(right)))
    go(remote(cotall.at[y, top], cotall.at[y, top], cot_s.at[3], cot_r.at[3], at_y(left)))
    go(remote(dsend, drecv, core_s.at[0], core_r.at[0], partner))
    tell_z()

    levels = code_ref.shape[0]
    code_t = code_ref[...].astype(F32)
    padding = jnp.zeros((size - levels, rows), F32)
    code = jnp.concatenate([code_t, padding], axis=0).T
    lane = lax.broadcasted_iota(jnp.int32, (1, size), 1)
    scale = jnp.zeros((1, size), F32)
    scales = [1.0 / math.sqrt(SPAN * 2 ** max(l - 1, 0)) for l in range(levels)]
    for l in range(levels):
        scale = jnp.where(lane == l, scales[l], scale)
    coefs = []
    for h in range(heads):
        lam = jnp.zeros((rows, size), F32)
        for entry in range(CODES):
            lam = jnp.where(code == float(entry), table_ref[h:h + 1, entry:entry + 1], lam)
        coefs.append(lam * scale)

    loads[3].wait()
    row = lax.broadcasted_iota(jnp.int32, (rows, rows), 0)
    column = lax.broadcasted_iota(jnp.int32, (rows, rows), 1)
    row_span, column_span = row // SPAN, column // SPAN
    in_level = [
        (row_span == column_span) & (column <= row),
        (row_span // 2 == column_span // 2) & (column_span < row_span),
        (row_span >= 2) & (column_span < 2),
    ]

    def local_forward(h):
        weight = jnp.zeros((rows, rows), F32)
        for l in range(3):
            weight = jnp.where(in_level[l], coefs[h][:, l:l + 1], weight)
        score = mm(q_ref[:, col(h)], k_ref[:, col(h)], NT)
        scores[h] = score
        lw[h] = weight
        prob = (score * weight).astype(BF16)
        probs[h] = prob
        attnl[:, col(h)] = mm(prob, v_ref[:, col(h)], NN)

    for h in range(2):
        local_forward(h)
    arrived(drecv, core_r.at[0])
    half_rows = pl.ds(pl.multiple_of(c * 256, 256), 256)
    zsend_f[...] = (dsend[half_rows, :].astype(F32) + drecv[half_rows, :].astype(F32)).astype(BF16)
    hear_z()
    for off in Z_ORDER:
        zt = mod(z + off, NZ)
        go(remote(zsend_f.at[pl.ds(pl.multiple_of(zt * 32, 32), 32)], zrecv_f.at[z],
                  zf_s.at[off], zf_r.at[off], at_z(zt)))
    own_slice = pl.ds(pl.multiple_of(z * 32, 32), 32)
    zrecv_f[z] = zsend_f[own_slice, :]

    for h in range(2, heads):
        local_forward(h)
    for h in range(heads):
        for l in range(3, levels):
            coefb[h, l - 3] = jnp.broadcast_to(coefs[h][:, l:l + 1], (rows, size))

    arrived(cotall.at[left, top], cot_r.at[0])
    go(remote(cotall.at[left, top], cotall.at[left, top], cot_s.at[4], cot_r.at[4], at_y(right)))
    arrived(cotall.at[right, low], cot_r.at[2])
    go(remote(cotall.at[right, low], cotall.at[right, low], cot_s.at[5], cot_r.at[5], at_y(left)))

    for off in range(1, NZ):
        arrived(zrecv_f.at[mod(z - off, NZ)], zf_r.at[off])
    parts = [zrecv_f[i].astype(F32) for i in range(NZ)]
    pairs = [parts[2 * i] + parts[2 * i + 1] for i in range(4)]
    quads = [pairs[0] + pairs[1], pairs[2] + pairs[3]]
    xsend_f[...] = (quads[0] + quads[1]).astype(BF16)
    for off in range(1, NX):
        xt = mod(x + off, NX)
        go(remote(xsend_f, xrecv_f.at[x], xf_s.at[off], xf_r.at[off], at_x(xt)), xt > x)
    for zt in range(NZ):
        if zt & 1:
            rsend_f[zt, 0] = parts[zt - 1].astype(BF16)
        if zt & 2:
            rsend_f[zt, 1] = pairs[2 * (zt // 4)].astype(BF16)
        if zt & 4:
            rsend_f[zt, 2] = quads[0].astype(BF16)
    for off in Z_ORDER:
        zt = mod(z + off, NZ)
        for l in range(3):
            go(remote(rsend_f.at[zt, l], fall.at[l, c, own_slice],
                      rf_s.at[off, l], rf_r.at[off, l], at_z(zt)), bit_of(zt, l) == 1)
    for l in range(3):
        @pl.when(level_bits[l] == 1)
        def _(l=l):
            fall[l, c, own_slice, :] = rsend_f[z, l]

    for off in range(1, NX):
        xs = mod(x - off, NX)
        arrived(xrecv_f.at[xs], xf_r.at[off], xs < x)

    @pl.when(bit_of(x, 0) == 1)
    def _():
        rx_f[0] = xrecv_f[x - 1]
        fall[3, c, own_slice, :] = xrecv_f[x - 1]

    @pl.when(x >= 2)
    def _():
        both = (xrecv_f[0].astype(F32) + xrecv_f[1].astype(F32)).astype(BF16)
        rx_f[1] = both
        fall[4, c, own_slice, :] = both

    for off in Z_ORDER:
        zt = mod(z + off, NZ)
        for l in range(3, 5):
            go(remote(rx_f.at[l - 3], fall.at[l, c, own_slice],
                      rf_s.at[off, l], rf_r.at[off, l], at_z(zt)), level_bits[l] == 1)

    loads[4].wait()
    opposite = mod(y + 2, 4)
    arrived(cotall.at[left, low], cot_r.at[1])
    arrived(cotall.at[right, top], cot_r.at[3])
    arrived(cotall.at[opposite, top], cot_r.at[4])
    arrived(cotall.at[opposite, low], cot_r.at[5])
    full_rows = jnp.concatenate([cotall[i] for i in range(4)], axis=1)
    gbuf[...] = mm(full_rows, w_ref[...], NT).astype(BF16)

    for h in range(heads):
        grad = gbuf[:, col(h)].astype(F32)
        for l in range(6):
            sgbuf[h, :, col(l)] = (coefb[h, l] * grad).astype(BF16)
        terms = mm(q_ref[:, col(h)], sgbuf[h], TN)
        t0send[col(h), :] = terms[:, col(0)].astype(BF16)
        for l in range(5):
            tsend[l, h // 2, col(h % 2), :] = terms[:, col(l + 1)].astype(BF16)
    go(remote(tsend.at[:, other], trecv, core_s.at[1], core_r.at[1], partner))
    go(remote(t0send, t0recv, core_s.at[2], core_r.at[2], partner))

    for off in range(1, NZ):
        zs = mod(z - off, NZ)
        zs_slice = pl.ds(pl.multiple_of(zs * 32, 32), 32)
        for l in range(5):
            arrived(fall.at[l, c, zs_slice], rf_r.at[off, l], level_bits[l] == 1)
    go(remote(fall.at[:, c], fall.at[:, c], core_s.at[3], core_r.at[3], partner))

    arrived(trecv, core_r.at[1])
    for l in range(5):
        zsend_b[l] = (tsend[l, c].astype(F32) + trecv[l].astype(F32)).astype(BF16)
    for off in Z_ORDER:
        zt = mod(z + off, NZ)
        for l in range(5):
            go(remote(zsend_b.at[l, pl.ds(pl.multiple_of(zt * 32, 32), 32)], zrecv_b.at[z, l],
                      zb_s.at[off, l], zb_r.at[off, l], at_z(zt)), level_bits[l] == 1)
    for l in range(5):
        @pl.when(level_bits[l] == 1)
        def _(l=l):
            zrecv_b[z, l] = zsend_b[l, own_slice, :]

    arrived(fall.at[:, other], core_r.at[3])

    def found_states(h):
        found = [jnp.where(c == 1, drecv[col(h), :], jnp.zeros((size, size), BF16))]
        found += [fall[l, h // 2, col(h % 2), :] for l in range(5)]
        return jnp.concatenate(found, axis=1)

    for h in range(heads):
        values = mm(q_ref[:, col(h)], found_states(h), NN)
        reads[h] = values
        attention = attnl[:, col(h)]
        for l in range(6):
            attention = attention + coefb[h, l] * values[:, col(l)]
        abuf[:, col(h)] = attention.astype(BF16)

    def weight_part(step, target):
        part = mm(cotall[target], abuf[...], TN)
        for block in range(16):
            wpart[target, block % 2, pl.ds((block // 2) * 32, 32), :] = (
                part[block * 32:(block + 1) * 32].astype(BF16)
            )
        go(remote(wpart.at[target, other], wrecv.at[target], wc_s.at[step], wc_r.at[step], partner))

    def weight_chip(step, target):
        arrived(wrecv.at[target], wc_r.at[step])
        wpart[target, c] = (wpart[target, c].astype(F32) + wrecv[target].astype(F32)).astype(BF16)

    def product_for(target):
        columns = pl.ds(pl.multiple_of(target * 512, 512), 512)
        mpart[target] = mm(abuf[...], w_ref[:, columns], NN).astype(BF16)

    sides = [pl.ds(128 * i, 128) for i in range(PIECES)]
    weight_part(0, x_opposite)
    product_for(opposite)
    go(remote(mpart.at[opposite, top], mrelay.at[0], m_s.at[0], m_r.at[0], at_y(left)))
    go(remote(mpart.at[opposite, low], mrelay.at[1], m_s.at[1], m_r.at[1], at_y(right)))
    weight_part(1, x_left)
    weight_chip(0, x_opposite)
    for i in range(PIECES):
        go(remote(wpart.at[x_opposite, c, top, sides[i]], wrelay.at[0, :, sides[i]],
                  wx_s.at[4 * i], wx_r.at[4 * i], at_x(x_left)))
        go(remote(wpart.at[x_opposite, c, low, sides[i]], wrelay.at[1, :, sides[i]],
                  wx_s.at[4 * i + 1], wx_r.at[4 * i + 1], at_x(x_right)))
    weight_part(2, x_right)
    product_for(left)
    product_for(right)
    entry_row = lax.broadcasted_iota(jnp.int32, (CODES, rows), 0).astype(F32)
    one_hot = [
        jnp.where(jnp.broadcast_to(code_t[l:l + 1, :], (CODES, rows)) == entry_row, 1.0, 0.0).astype(BF16)
        for l in range(levels)
    ]
    table_parts = []

    def local_back(h):
        grad = gbuf[:, col(h)]
        prob_grad = mm(grad, v_ref[:, col(h)], NT)
        score_grad = (prob_grad * lw[h]).astype(BF16)
        product = scores[h] * prob_grad
        total = jnp.zeros((CODES, rows), F32)
        for l in range(3):
            masked = jnp.where(in_level[l], product, 0.0).astype(BF16)
            total = total + scales[l] * mm(one_hot[l], masked, NN)
        qgl[:, col(h)] = mm(score_grad, k_ref[:, col(h)], NN)
        kgl[:, col(h)] = mm(score_grad, q_ref[:, col(h)], TN)
        vgl[:, col(h)] = mm(probs[h], grad, TN)
        table_parts.append(total[:, :size] + total[:, size:])

    for h in range(3):
        local_back(h)

    weight_chip(1, x_left)
    weight_chip(2, x_right)

    def weight_relay(i):
        side = sides[i]
        arrived(wrelay.at[0, :, side], wx_r.at[4 * i])
        wpart[x_left, c, top, side] = (
            wpart[x_left, c, top, side].astype(F32) + wrelay[0, :, side].astype(F32)
        ).astype(BF16)
        go(remote(wpart.at[x_left, c, :, side], wxrecv.at[0, :, side],
                  wx_s.at[4 * i + 2], wx_r.at[4 * i + 2], at_x(x_left)))
        arrived(wrelay.at[1, :, side], wx_r.at[4 * i + 1])
        wpart[x_right, c, low, side] = (
            wpart[x_right, c, low, side].astype(F32) + wrelay[1, :, side].astype(F32)
        ).astype(BF16)
        go(remote(wpart.at[x_right, c, :, side], wxrecv.at[1, :, side],
                  wx_s.at[4 * i + 3], wx_r.at[4 * i + 3], at_x(x_right)))

    weight_relay(0)
    for off in range(1, NZ):
        zs = mod(z - off, NZ)
        for l in range(5):
            bit = bit_of(zs, l) if l < 3 else level_bits[l]
            arrived(zrecv_b.at[zs, l], zb_r.at[off, l], bit == 1)
    for l in range(2):
        @pl.when(level_bits[3 + l] == 1)
        def _(l=l):
            ring = zrecv_b[0, 3 + l].astype(F32)
            for zs in range(1, NZ):
                ring = ring + zrecv_b[zs, 3 + l].astype(F32)
            xsend_b[l] = ring.astype(BF16)
    for off in range(1, NX):
        xt = mod(x + off, NX)
        bit = jnp.where(lax.div(x, 2) == lax.div(xt, 2), 0, 1)
        go(remote(xsend_b.at[bit], xrecv_b.at[x], xb_s.at[off], xb_r.at[off], at_x(xt)), xt < x)

    local_back(3)
    weight_relay(1)
    weight_part(3, x)
    product_for(y)
    for i in range(2, PIECES):
        weight_relay(i)

    for off in range(1, NX):
        xs = mod(x - off, NX)
        arrived(xrecv_b.at[xs], xb_r.at[off], xs > x)
    from_x = jnp.zeros((32, size), F32)
    for xs in range(1, NX):
        from_x = from_x + jnp.where(x < xs, xrecv_b[xs].astype(F32), 0.0)
    quad = zrecv_b[4, 2].astype(F32)
    for zs in range(5, NZ):
        quad = quad + zrecv_b[zs, 2].astype(F32)
    for zt in range(NZ):
        total = from_x
        if zt & 1 == 0:
            total = total + zrecv_b[zt + 1, 0].astype(F32)
        if zt & 2 == 0:
            upper = (zt // 4) * 4 + 2
            total = total + zrecv_b[upper, 1].astype(F32) + zrecv_b[upper + 1, 1].astype(F32)
        if zt & 4 == 0:
            total = total + quad
        gsend[zt] = total.astype(BF16)
    for off in Z_ORDER:
        zt = mod(z + off, NZ)
        go(remote(gsend.at[zt], gall.at[c, own_slice], rb_s.at[off], rb_r.at[off], at_z(zt)))
    gall[c, own_slice, :] = gsend[z]

    def weight_ring(i):
        side = sides[i]
        arrived(wxrecv.at[0, :, side], wx_r.at[4 * i + 2])
        arrived(wxrecv.at[1, :, side], wx_r.at[4 * i + 3])
        wz[:, side] = (
            wpart[x, c, :, side].astype(F32) + wxrecv[0, :, side].astype(F32) + wxrecv[1, :, side].astype(F32)
        ).astype(BF16)
        for off in Z_ORDER:
            zt = mod(z + off, NZ)
            go(remote(wz.at[pl.ds(pl.multiple_of(zt * 32, 32), 32), side], wzrecv.at[z, :, side],
                      wz_s.at[off, i], wz_r.at[off, i], at_z(zt)))
        wzrecv[z, :, side] = wz[own_slice, side]

    weight_chip(3, x)
    weight_ring(0)
    arrived(mrelay.at[0], m_r.at[0])
    mpart[left, top] = (mpart[left, top].astype(F32) + mrelay[0].astype(F32)).astype(BF16)
    go(remote(mpart.at[left], mrecv.at[0], m_s.at[2], m_r.at[2], at_y(left)))
    arrived(mrelay.at[1], m_r.at[1])
    mpart[right, low] = (mpart[right, low].astype(F32) + mrelay[1].astype(F32)).astype(BF16)
    go(remote(mpart.at[right], mrecv.at[1], m_s.at[3], m_r.at[3], at_y(right)))

    for h in range(heads):
        grad = gbuf[:, col(h)].astype(F32)
        total = table_parts[h]
        for l in range(6):
            total = total + scales[l + 3] * mm(one_hot[l + 3], (grad * reads[h, :, col(l)]).astype(BF16), NN)
        table_parts[h] = total
        qg_ref[:, col(h)] = (qgl[:, col(h)] + mm(sgbuf[h], found_states(h), NT)).astype(BF16)
    lane128 = lax.broadcasted_iota(jnp.int32, (CODES, size), 1)
    partial_table = jnp.zeros((CODES, size), F32)
    for h in range(heads):
        summed = jnp.sum(table_parts[h], axis=1, keepdims=True)
        partial_table = jnp.where(lane128 == h, summed, partial_table)
    tgsend[...] = partial_table
    go(remote(tgsend, tgcore, core_s.at[4], core_r.at[4], partner))

    weight_ring(1)
    arrived(tgcore, core_r.at[4])
    tgzsend[...] = tgsend[...] + tgcore[...]
    for off in range(1, NZ):
        go(remote(tgzsend, tgz.at[z], tz_s.at[off], tz_r.at[off], at_z(mod(z + off, NZ))))
    tgz[z] = tgzsend[...]

    for i in range(2, PIECES):
        weight_ring(i)

    for off in range(1, NZ):
        zs = mod(z - off, NZ)
        arrived(gall.at[c, pl.ds(pl.multiple_of(zs * 32, 32), 32)], rb_r.at[off])
    go(remote(gall.at[c], gall.at[c], core_s.at[5], core_r.at[5], partner))
    for off in range(1, NZ):
        arrived(tgz.at[mod(z - off, NZ)], tz_r.at[off])
    ring_table = tgz[0]
    for zs in range(1, NZ):
        ring_table = ring_table + tgz[zs]
    tgxsend[...] = ring_table
    for off in range(1, NX):
        go(remote(tgxsend, tgx.at[x], tx_s.at[off], tx_r.at[off], at_x(mod(x + off, NX))))
    tgx[x] = ring_table

    arrived(gall.at[other], core_r.at[5])
    arrived(t0recv, core_r.at[2])
    for h in range(heads):
        back = gall[h // 2, col(h % 2), :].astype(F32) + jnp.where(c == 0, t0recv[col(h), :].astype(F32), 0.0)
        back = back.astype(BF16)
        kg_ref[:, col(h)] = (kgl[:, col(h)] + mm(v_ref[:, col(h)], back, NT)).astype(BF16)
        vg_ref[:, col(h)] = (vgl[:, col(h)] + mm(k_ref[:, col(h)], back, NN)).astype(BF16)

    arrived(mrecv.at[0], m_r.at[2])
    arrived(mrecv.at[1], m_r.at[3])
    mixed_ref[...] = (
        mpart[y].astype(F32) + mrecv[0].astype(F32) + mrecv[1].astype(F32)
    ).astype(BF16)

    for off in range(1, NX):
        arrived(tgx.at[mod(x - off, NX)], tx_r.at[off])
    table = tgx[0]
    for xs in range(1, NX):
        table = table + tgx[xs]
    tokens = rows * 2 * NZ * NX
    square = jnp.concatenate([table, jnp.zeros((size - CODES, size), F32)], axis=0)
    tg_ref[...] = square.T[:heads, :CODES] * (1.0 / math.sqrt(tokens * levels))

    for i in range(PIECES):
        for off in range(1, NZ):
            arrived(wzrecv.at[mod(z - off, NZ), :, sides[i]], wz_r.at[off, i])
        weight = wzrecv[0, :, sides[i]].astype(F32)
        for zs in range(1, NZ):
            weight = weight + wzrecv[zs, :, sides[i]].astype(F32)
        wg_ref[:, sides[i]] = weight * (1.0 / math.sqrt(tokens))

    for copy, cond in pending:
        if cond is None:
            copy.wait_send()
        else:
            pl.when(cond)(lambda copy=copy: copy.wait_send())


def store(*refs):
    sources, targets, sems = refs[:6], refs[6:12], refs[12]
    copies = [
        pltpu.make_async_copy(source, target, sems.at[i])
        for i, (source, target) in enumerate(zip(sources, targets))
    ]
    for copy in copies:
        copy.start()
    for copy in copies:
        copy.wait()


def per_device(queries, keys, values, level_table, level_code, out_weight, cotangent):
    rows, width = queries.shape
    vmem = pl.BlockSpec(memory_space=pltpu.VMEM)
    hbm = pl.BlockSpec(memory_space=pltpu.MemorySpace.HBM)
    dma = pltpu.SemaphoreType.DMA

    def bf(*shape):
        return pltpu.VMEM(shape, BF16)

    def f32(*shape):
        return pltpu.VMEM(shape, F32)

    scratch = [
        bf(rows, 512), bf(rows, 512), bf(rows, 512), bf(512, 2048), dma((5,)),
        pltpu.SemaphoreType.REGULAR((2,)), f32(4, rows, 768), bf(4, rows, 512), f32(4, 6, rows, 128), f32(4, rows, rows), f32(4, rows, rows),
        bf(4, rows, rows), bf(4, rows, 768), bf(rows, 512), bf(rows, 512),
        f32(rows, 512), f32(rows, 512), f32(rows, 512), f32(rows, 512),
        bf(512, 128), bf(512, 128), bf(256, 128), bf(NZ, 32, 128), bf(32, 128), bf(NX, 32, 128),
        bf(NZ, 3, 32, 128), bf(2, 32, 128), bf(5, 2, 256, 128),
        bf(512, 128), bf(512, 128), bf(5, 2, 256, 128), bf(5, 256, 128), bf(5, 256, 128),
        bf(NZ, 5, 32, 128), bf(2, 32, 128), bf(NX, 32, 128), bf(NZ, 32, 128), bf(2, 256, 128),
        bf(4, rows, 512), bf(2, rows // 2, 512), bf(2, rows, 512),
        bf(4, 2, 256, 512), bf(4, 256, 512), bf(2, 128, 512), bf(2, 256, 512), bf(256, 512),
        bf(NZ, 32, 512),
        f32(CODES, 128), f32(CODES, 128), f32(CODES, 128), f32(NZ, CODES, 128),
        f32(CODES, 128), f32(NX, CODES, 128),
        dma((6,)), dma((6,)), dma((6,)), dma((6,)), dma((NZ,)), dma((NZ,)), dma((NX,)), dma((NX,)),
        dma((NZ, 5)), dma((NZ, 5)), dma((NZ, 5)), dma((NZ, 5)), dma((NX,)), dma((NX,)),
        dma((NZ,)), dma((NZ,)), dma((4,)), dma((4,)), dma((4,)), dma((4,)), dma((4 * PIECES,)), dma((4 * PIECES,)),
        dma((NZ, PIECES)), dma((NZ, PIECES)), dma((NZ,)), dma((NZ,)), dma((NX,)), dma((NX,)),
    ]
    shape = jax.ShapeDtypeStruct
    results = pl.pallas_call(
        kernel,
        out_shape=(
            shape((rows, width), BF16),
            shape((32, width), F32),
            shape((rows, width), BF16),
            shape((rows, width), BF16),
            shape((rows, width), BF16),
            shape((4, CODES), F32),
        ),
        in_specs=[hbm, hbm, hbm, vmem, vmem, hbm, hbm],
        out_specs=[vmem] * 6,
        scratch_shapes=scratch,
        compiler_params=pltpu.CompilerParams(
            collective_id=0, has_side_effects=True, vmem_limit_bytes=53900 * 2**10
        ),
        name="layer",
    )(queries, keys, values, level_table.T, level_code.T, out_weight, cotangent)
    stored = pl.pallas_call(
        store,
        out_shape=tuple(shape(value.shape, value.dtype) for value in results),
        in_specs=[vmem] * 6,
        out_specs=[pl.BlockSpec(memory_space=pl.ANY)] * 6,
        scratch_shapes=[dma((6,))],
        compiler_params=pltpu.CompilerParams(vmem_limit_bytes=2**20),
        name="store",
    )(*results)
    return (*stored[:5], stored[5].T)


def solution(mesh):
    wide = P("seq", "head")
    return jax.shard_map(
        per_device,
        mesh=mesh,
        in_specs=(wide, wide, wide, P(None, "head"), P("seq", None), P("head", None), wide),
        out_specs=(wide, wide, wide, wide, wide, P(None, "head")),
        check_vma=False,
    )
```

```python
import math

import jax
import jax.numpy as jnp
from jax import lax
from jax.experimental import pallas as pl
from jax.experimental.pallas import tpu as pltpu
from jax.sharding import PartitionSpec as P

SPAN = 64
CODES = 16
NX, NZ = 4, 8
Z_ORDER = (4, 3, 5, 2, 6, 1, 7)
PIECES = 4
F32, BF16 = jnp.float32, jnp.bfloat16
MESH = pl.DeviceIdType.MESH
NN = (((1,), (0,)), ((), ()))
NT = (((1,), (1,)), ((), ()))
TN = (((0,), (0,)), ((), ()))


def mm(left, right, dims):
    return lax.dot_general(left, right, dims, preferred_element_type=F32)


def remote(src, dst, send_sem, recv_sem, device):
    return pltpu.make_async_remote_copy(
        src_ref=src,
        dst_ref=dst,
        send_sem=send_sem,
        recv_sem=recv_sem,
        device_id=device,
        device_id_type=MESH,
    )


def mod(value, size):
    return lax.rem(value + size, size)


def bit_of(value, index):
    return lax.rem(lax.div(value, 2**index), 2)


def kernel(
    q_hbm, k_hbm, v_hbm, table_ref, code_ref, w_hbm, cot_hbm,
    mixed_ref, wg_ref, qg_ref, kg_ref, vg_ref, tg_ref,
    q_ref, k_ref, v_ref, w_ref, load_sems, far_sems, reads, cotall, coefb, scores, lw, probs, sgbuf, gbuf, abuf, attnl, qgl, kgl, vgl,
    dsend, drecv, zsend_f, zrecv_f, xsend_f, xrecv_f, rsend_f, rx_f, fall,
    t0send, t0recv, tsend, trecv, zsend_b, zrecv_b, xsend_b, xrecv_b, gsend, gall,
    mpart, mrelay, mrecv, wpart, wrecv, wrelay, wxrecv, wz, wzrecv,
    tgsend, tgcore, tgzsend, tgz, tgxsend, tgx,
    cot_s, cot_r, core_s, core_r, zf_s, zf_r, xf_s, xf_r, rf_s, rf_r,
    zb_s, zb_r, xb_s, xb_r, rb_s, rb_r, m_s, m_r, wc_s, wc_r, wx_s, wx_r, wz_s, wz_r,
    tz_s, tz_r, tx_s, tx_r,
):
    s = lax.axis_index("seq")
    y = lax.axis_index("head")
    c = lax.rem(s, 2)
    z = lax.rem(lax.div(s, 2), NZ)
    x = lax.div(s, 2 * NZ)
    other = 1 - c
    heads, size = 4, 128
    rows = q_ref.shape[0]
    loads = [
        pltpu.make_async_copy(source, target, load_sems.at[i])
        for i, (source, target) in enumerate(
            [(cot_hbm, cotall.at[y]), (k_hbm, k_ref), (v_hbm, v_ref), (q_hbm, q_ref), (w_hbm, w_ref)]
        )
    ]
    for load in loads:
        load.start()
    half = rows // 2

    def at_y(target):
        return (s, target)

    def at_z(target):
        return ((x * NZ + target) * 2 + c, y)

    def at_x(target):
        return ((target * NZ + z) * 2 + c, y)

    partner = (s + 1 - 2 * c, y)
    level_bits = [bit_of(z, 0), bit_of(z, 1), bit_of(z, 2), bit_of(x, 0), bit_of(x, 1)]
    pending = []

    def go(copy, cond=None):
        pending.append((copy, cond))
        if cond is None:
            copy.start()
        else:
            pl.when(cond)(lambda: copy.start())

    def arrived(dst, sem, cond=None):
        copy = remote(dst, dst, sem, sem, partner)
        if cond is None:
            copy.wait_recv()
        else:
            pl.when(cond)(lambda: copy.wait_recv())

    def col(h):
        return slice(h * size, (h + 1) * size)

    right, left = mod(y + 1, 4), mod(y - 1, 4)
    x_right, x_left, x_opposite = mod(x + 1, 4), mod(x - 1, 4), mod(x + 2, 4)
    barrier = pltpu.get_barrier_semaphore()
    near = [partner, at_y(right), at_y(left), at_x(x_right), at_x(x_left), at_x(x_opposite)]
    near += [at_z(mod(z + off, NZ)) for off in (1, -1, 2, -2)]
    for device in near:
        pl.semaphore_signal(barrier, inc=1, device_id=device, device_id_type=MESH)

    def tell(index, device):
        pl.semaphore_signal(far_sems.at[index], inc=1, device_id=device, device_id_type=MESH)

    def tell_z():
        tell(0, at_z(mod(z + 2, NZ)))
        tell(1, at_z(mod(z - 2, NZ)))

    def hear_z():
        pl.semaphore_wait(far_sems.at[0], 1)
        pl.semaphore_wait(far_sems.at[1], 1)

    loads[1].wait()
    loads[2].wait()
    for h in range(heads):
        dsend[col(h), :] = mm(k_ref[:, col(h)], v_ref[:, col(h)], TN).astype(BF16)
    for l in range(5):
        @pl.when(level_bits[l] == 0)
        def _(l=l):
            fall[l, c] = jnp.zeros((256, size), BF16)
    loads[0].wait()
    pl.semaphore_wait(barrier, len(near))

    top, low = pl.ds(0, half), pl.ds(half, half)
    go(remote(cotall.at[y, top], cotall.at[y, top], cot_s.at[0], cot_r.at[0], at_y(right)))
    go(remote(cotall.at[y, low], cotall.at[y, low], cot_s.at[2], cot_r.at[2], at_y(left)))
    go(remote(cotall.at[y, low], cotall.at[y, low], cot_s.at[1], cot_r.at[1], at_y(right)))
    go(remote(cotall.at[y, top], cotall.at[y, top], cot_s.at[3], cot_r.at[3], at_y(left)))
    go(remote(dsend, drecv, core_s.at[0], core_r.at[0], partner))
    tell_z()

    levels = code_ref.shape[0]
    code_t = code_ref[...].astype(F32)
    padding = jnp.zeros((size - levels, rows), F32)
    code = jnp.concatenate([code_t, padding], axis=0).T
    lane = lax.broadcasted_iota(jnp.int32, (1, size), 1)
    scale = jnp.zeros((1, size), F32)
    scales = [1.0 / math.sqrt(SPAN * 2 ** max(l - 1, 0)) for l in range(levels)]
    for l in range(levels):
        scale = jnp.where(lane == l, scales[l], scale)
    coefs = []
    for h in range(heads):
        lam = jnp.zeros((rows, size), F32)
        for entry in range(CODES):
            lam = jnp.where(code == float(entry), table_ref[h:h + 1, entry:entry + 1], lam)
        coefs.append(lam * scale)

    loads[3].wait()
    row = lax.broadcasted_iota(jnp.int32, (rows, rows), 0)
    column = lax.broadcasted_iota(jnp.int32, (rows, rows), 1)
    row_span, column_span = row // SPAN, column // SPAN
    in_level = [
        (row_span == column_span) & (column <= row),
        (row_span // 2 == column_span // 2) & (column_span < row_span),
        (row_span >= 2) & (column_span < 2),
    ]

    def local_forward(h):
        weight = jnp.zeros((rows, rows), F32)
        for l in range(3):
            weight = jnp.where(in_level[l], coefs[h][:, l:l + 1], weight)
        score = mm(q_ref[:, col(h)], k_ref[:, col(h)], NT)
        scores[h] = score
        lw[h] = weight
        prob = (score * weight).astype(BF16)
        probs[h] = prob
        attnl[:, col(h)] = mm(prob, v_ref[:, col(h)], NN)

    for h in range(2):
        local_forward(h)
    arrived(drecv, core_r.at[0])
    half_rows = pl.ds(pl.multiple_of(c * 256, 256), 256)
    zsend_f[...] = (dsend[half_rows, :].astype(F32) + drecv[half_rows, :].astype(F32)).astype(BF16)
    hear_z()
    for off in Z_ORDER:
        zt = mod(z + off, NZ)
        go(remote(zsend_f.at[pl.ds(pl.multiple_of(zt * 32, 32), 32)], zrecv_f.at[z],
                  zf_s.at[off], zf_r.at[off], at_z(zt)))
    own_slice = pl.ds(pl.multiple_of(z * 32, 32), 32)
    zrecv_f[z] = zsend_f[own_slice, :]

    for h in range(2, heads):
        local_forward(h)
    for h in range(heads):
        for l in range(3, levels):
            coefb[h, l - 3] = jnp.broadcast_to(coefs[h][:, l:l + 1], (rows, size))

    arrived(cotall.at[left, top], cot_r.at[0])
    go(remote(cotall.at[left, top], cotall.at[left, top], cot_s.at[4], cot_r.at[4], at_y(right)))
    arrived(cotall.at[right, low], cot_r.at[2])
    go(remote(cotall.at[right, low], cotall.at[right, low], cot_s.at[5], cot_r.at[5], at_y(left)))

    for off in range(1, NZ):
        arrived(zrecv_f.at[mod(z - off, NZ)], zf_r.at[off])
    parts = [zrecv_f[i].astype(F32) for i in range(NZ)]
    pairs = [parts[2 * i] + parts[2 * i + 1] for i in range(4)]
    quads = [pairs[0] + pairs[1], pairs[2] + pairs[3]]
    xsend_f[...] = (quads[0] + quads[1]).astype(BF16)
    for off in range(1, NX):
        xt = mod(x + off, NX)
        go(remote(xsend_f, xrecv_f.at[x], xf_s.at[off], xf_r.at[off], at_x(xt)), xt > x)
    for zt in range(NZ):
        if zt & 1:
            rsend_f[zt, 0] = parts[zt - 1].astype(BF16)
        if zt & 2:
            rsend_f[zt, 1] = pairs[2 * (zt // 4)].astype(BF16)
        if zt & 4:
            rsend_f[zt, 2] = quads[0].astype(BF16)
    for off in Z_ORDER:
        zt = mod(z + off, NZ)
        for l in range(3):
            go(remote(rsend_f.at[zt, l], fall.at[l, c, own_slice],
                      rf_s.at[off, l], rf_r.at[off, l], at_z(zt)), bit_of(zt, l) == 1)
    for l in range(3):
        @pl.when(level_bits[l] == 1)
        def _(l=l):
            fall[l, c, own_slice, :] = rsend_f[z, l]

    for off in range(1, NX):
        xs = mod(x - off, NX)
        arrived(xrecv_f.at[xs], xf_r.at[off], xs < x)

    @pl.when(bit_of(x, 0) == 1)
    def _():
        rx_f[0] = xrecv_f[x - 1]
        fall[3, c, own_slice, :] = xrecv_f[x - 1]

    @pl.when(x >= 2)
    def _():
        both = (xrecv_f[0].astype(F32) + xrecv_f[1].astype(F32)).astype(BF16)
        rx_f[1] = both
        fall[4, c, own_slice, :] = both

    for off in Z_ORDER:
        zt = mod(z + off, NZ)
        for l in range(3, 5):
            go(remote(rx_f.at[l - 3], fall.at[l, c, own_slice],
                      rf_s.at[off, l], rf_r.at[off, l], at_z(zt)), level_bits[l] == 1)

    loads[4].wait()
    opposite = mod(y + 2, 4)
    arrived(cotall.at[left, low], cot_r.at[1])
    arrived(cotall.at[right, top], cot_r.at[3])
    arrived(cotall.at[opposite, top], cot_r.at[4])
    arrived(cotall.at[opposite, low], cot_r.at[5])
    full_rows = jnp.concatenate([cotall[i] for i in range(4)], axis=1)
    gbuf[...] = mm(full_rows, w_ref[...], NT).astype(BF16)

    for h in range(heads):
        grad = gbuf[:, col(h)].astype(F32)
        for l in range(6):
            sgbuf[h, :, col(l)] = (coefb[h, l] * grad).astype(BF16)
        terms = mm(q_ref[:, col(h)], sgbuf[h], TN)
        t0send[col(h), :] = terms[:, col(0)].astype(BF16)
        for l in range(5):
            tsend[l, h // 2, col(h % 2), :] = terms[:, col(l + 1)].astype(BF16)
    go(remote(tsend.at[:, other], trecv, core_s.at[1], core_r.at[1], partner))
    go(remote(t0send, t0recv, core_s.at[2], core_r.at[2], partner))

    for off in range(1, NZ):
        zs = mod(z - off, NZ)
        zs_slice = pl.ds(pl.multiple_of(zs * 32, 32), 32)
        for l in range(5):
            arrived(fall.at[l, c, zs_slice], rf_r.at[off, l], level_bits[l] == 1)
    go(remote(fall.at[:, c], fall.at[:, c], core_s.at[3], core_r.at[3], partner))

    arrived(trecv, core_r.at[1])
    for l in range(5):
        zsend_b[l] = (tsend[l, c].astype(F32) + trecv[l].astype(F32)).astype(BF16)
    for off in Z_ORDER:
        zt = mod(z + off, NZ)
        for l in range(5):
            go(remote(zsend_b.at[l, pl.ds(pl.multiple_of(zt * 32, 32), 32)], zrecv_b.at[z, l],
                      zb_s.at[off, l], zb_r.at[off, l], at_z(zt)), level_bits[l] == 1)
    for l in range(5):
        @pl.when(level_bits[l] == 1)
        def _(l=l):
            zrecv_b[z, l] = zsend_b[l, own_slice, :]

    arrived(fall.at[:, other], core_r.at[3])

    def found_states(h):
        found = [jnp.where(c == 1, drecv[col(h), :], jnp.zeros((size, size), BF16))]
        found += [fall[l, h // 2, col(h % 2), :] for l in range(5)]
        return jnp.concatenate(found, axis=1)

    for h in range(heads):
        values = mm(q_ref[:, col(h)], found_states(h), NN)
        reads[h] = values
        attention = attnl[:, col(h)]
        for l in range(6):
            attention = attention + coefb[h, l] * values[:, col(l)]
        abuf[:, col(h)] = attention.astype(BF16)

    def weight_part(step, target):
        part = mm(cotall[target], abuf[...], TN)
        for block in range(16):
            wpart[target, block % 2, pl.ds((block // 2) * 32, 32), :] = (
                part[block * 32:(block + 1) * 32].astype(BF16)
            )
        go(remote(wpart.at[target, other], wrecv.at[target], wc_s.at[step], wc_r.at[step], partner))

    def weight_chip(step, target):
        arrived(wrecv.at[target], wc_r.at[step])
        wpart[target, c] = (wpart[target, c].astype(F32) + wrecv[target].astype(F32)).astype(BF16)

    def product_for(target):
        columns = pl.ds(pl.multiple_of(target * 512, 512), 512)
        mpart[target] = mm(abuf[...], w_ref[:, columns], NN).astype(BF16)

    sides = [pl.ds(128 * i, 128) for i in range(PIECES)]
    weight_part(0, x_opposite)
    product_for(opposite)
    go(remote(mpart.at[opposite, top], mrelay.at[0], m_s.at[0], m_r.at[0], at_y(left)))
    go(remote(mpart.at[opposite, low], mrelay.at[1], m_s.at[1], m_r.at[1], at_y(right)))
    weight_part(1, x_left)
    weight_chip(0, x_opposite)
    for i in range(PIECES):
        go(remote(wpart.at[x_opposite, c, top, sides[i]], wrelay.at[0, :, sides[i]],
                  wx_s.at[4 * i], wx_r.at[4 * i], at_x(x_left)))
        go(remote(wpart.at[x_opposite, c, low, sides[i]], wrelay.at[1, :, sides[i]],
                  wx_s.at[4 * i + 1], wx_r.at[4 * i + 1], at_x(x_right)))
    weight_part(2, x_right)
    product_for(left)
    product_for(right)
    entry_row = lax.broadcasted_iota(jnp.int32, (CODES, rows), 0).astype(F32)
    one_hot = [
        jnp.where(jnp.broadcast_to(code_t[l:l + 1, :], (CODES, rows)) == entry_row, 1.0, 0.0).astype(BF16)
        for l in range(levels)
    ]
    table_parts = []

    def local_back(h):
        grad = gbuf[:, col(h)]
        prob_grad = mm(grad, v_ref[:, col(h)], NT)
        score_grad = (prob_grad * lw[h]).astype(BF16)
        product = scores[h] * prob_grad
        total = jnp.zeros((CODES, rows), F32)
        for l in range(3):
            masked = jnp.where(in_level[l], product, 0.0).astype(BF16)
            total = total + scales[l] * mm(one_hot[l], masked, NN)
        qgl[:, col(h)] = mm(score_grad, k_ref[:, col(h)], NN)
        kgl[:, col(h)] = mm(score_grad, q_ref[:, col(h)], TN)
        vgl[:, col(h)] = mm(probs[h], grad, TN)
        table_parts.append(total[:, :size] + total[:, size:])

    for h in range(3):
        local_back(h)

    weight_chip(1, x_left)
    weight_chip(2, x_right)

    def weight_relay(i):
        side = sides[i]
        arrived(wrelay.at[0, :, side], wx_r.at[4 * i])
        wpart[x_left, c, top, side] = (
            wpart[x_left, c, top, side].astype(F32) + wrelay[0, :, side].astype(F32)
        ).astype(BF16)
        go(remote(wpart.at[x_left, c, :, side], wxrecv.at[0, :, side],
                  wx_s.at[4 * i + 2], wx_r.at[4 * i + 2], at_x(x_left)))
        arrived(wrelay.at[1, :, side], wx_r.at[4 * i + 1])
        wpart[x_right, c, low, side] = (
            wpart[x_right, c, low, side].astype(F32) + wrelay[1, :, side].astype(F32)
        ).astype(BF16)
        go(remote(wpart.at[x_right, c, :, side], wxrecv.at[1, :, side],
                  wx_s.at[4 * i + 3], wx_r.at[4 * i + 3], at_x(x_right)))

    weight_relay(0)
    for off in range(1, NZ):
        zs = mod(z - off, NZ)
        for l in range(5):
            bit = bit_of(zs, l) if l < 3 else level_bits[l]
            arrived(zrecv_b.at[zs, l], zb_r.at[off, l], bit == 1)
    for l in range(2):
        @pl.when(level_bits[3 + l] == 1)
        def _(l=l):
            ring = zrecv_b[0, 3 + l].astype(F32)
            for zs in range(1, NZ):
                ring = ring + zrecv_b[zs, 3 + l].astype(F32)
            xsend_b[l] = ring.astype(BF16)
    for off in range(1, NX):
        xt = mod(x + off, NX)
        bit = jnp.where(lax.div(x, 2) == lax.div(xt, 2), 0, 1)
        go(remote(xsend_b.at[bit], xrecv_b.at[x], xb_s.at[off], xb_r.at[off], at_x(xt)), xt < x)

    local_back(3)
    weight_relay(1)
    for h in range(heads):
        grad = gbuf[:, col(h)].astype(F32)
        total = table_parts[h]
        for l in range(6):
            total = total + scales[l + 3] * mm(one_hot[l + 3], (grad * reads[h, :, col(l)]).astype(BF16), NN)
        table_parts[h] = total
    lane128 = lax.broadcasted_iota(jnp.int32, (CODES, size), 1)
    partial_table = jnp.zeros((CODES, size), F32)
    for h in range(heads):
        summed = jnp.sum(table_parts[h], axis=1, keepdims=True)
        partial_table = jnp.where(lane128 == h, summed, partial_table)
    tgsend[...] = partial_table
    go(remote(tgsend, tgcore, core_s.at[4], core_r.at[4], partner))

    for i in range(2, PIECES):
        weight_relay(i)

    weight_part(3, x)
    product_for(y)
    for off in range(1, NX):
        xs = mod(x - off, NX)
        arrived(xrecv_b.at[xs], xb_r.at[off], xs > x)
    from_x = jnp.zeros((32, size), F32)
    for xs in range(1, NX):
        from_x = from_x + jnp.where(x < xs, xrecv_b[xs].astype(F32), 0.0)
    quad = zrecv_b[4, 2].astype(F32)
    for zs in range(5, NZ):
        quad = quad + zrecv_b[zs, 2].astype(F32)
    for zt in range(NZ):
        total = from_x
        if zt & 1 == 0:
            total = total + zrecv_b[zt + 1, 0].astype(F32)
        if zt & 2 == 0:
            upper = (zt // 4) * 4 + 2
            total = total + zrecv_b[upper, 1].astype(F32) + zrecv_b[upper + 1, 1].astype(F32)
        if zt & 4 == 0:
            total = total + quad
        gsend[zt] = total.astype(BF16)
    for off in Z_ORDER:
        zt = mod(z + off, NZ)
        go(remote(gsend.at[zt], gall.at[c, own_slice], rb_s.at[off], rb_r.at[off], at_z(zt)))
    gall[c, own_slice, :] = gsend[z]

    arrived(tgcore, core_r.at[4])
    tgzsend[...] = tgsend[...] + tgcore[...]
    for off in range(1, NZ):
        go(remote(tgzsend, tgz.at[z], tz_s.at[off], tz_r.at[off], at_z(mod(z + off, NZ))))
    tgz[z] = tgzsend[...]

    def weight_ring(i):
        side = sides[i]
        arrived(wxrecv.at[0, :, side], wx_r.at[4 * i + 2])
        arrived(wxrecv.at[1, :, side], wx_r.at[4 * i + 3])
        wz[:, side] = (
            wpart[x, c, :, side].astype(F32) + wxrecv[0, :, side].astype(F32) + wxrecv[1, :, side].astype(F32)
        ).astype(BF16)
        for off in Z_ORDER:
            zt = mod(z + off, NZ)
            go(remote(wz.at[pl.ds(pl.multiple_of(zt * 32, 32), 32), side], wzrecv.at[z, :, side],
                      wz_s.at[off, i], wz_r.at[off, i], at_z(zt)))
        wzrecv[z, :, side] = wz[own_slice, side]

    weight_chip(3, x)
    weight_ring(0)
    arrived(mrelay.at[0], m_r.at[0])
    mpart[left, top] = (mpart[left, top].astype(F32) + mrelay[0].astype(F32)).astype(BF16)
    go(remote(mpart.at[left], mrecv.at[0], m_s.at[2], m_r.at[2], at_y(left)))
    arrived(mrelay.at[1], m_r.at[1])
    mpart[right, low] = (mpart[right, low].astype(F32) + mrelay[1].astype(F32)).astype(BF16)
    go(remote(mpart.at[right], mrecv.at[1], m_s.at[3], m_r.at[3], at_y(right)))

    for h in range(heads):
        qg_ref[:, col(h)] = (qgl[:, col(h)] + mm(sgbuf[h], found_states(h), NT)).astype(BF16)

    weight_ring(1)
    for i in range(2, PIECES):
        weight_ring(i)

    for off in range(1, NZ):
        zs = mod(z - off, NZ)
        arrived(gall.at[c, pl.ds(pl.multiple_of(zs * 32, 32), 32)], rb_r.at[off])
    go(remote(gall.at[c], gall.at[c], core_s.at[5], core_r.at[5], partner))
    for off in range(1, NZ):
        arrived(tgz.at[mod(z - off, NZ)], tz_r.at[off])
    ring_table = tgz[0]
    for zs in range(1, NZ):
        ring_table = ring_table + tgz[zs]
    tgxsend[...] = ring_table
    for off in range(1, NX):
        go(remote(tgxsend, tgx.at[x], tx_s.at[off], tx_r.at[off], at_x(mod(x + off, NX))))
    tgx[x] = ring_table

    arrived(gall.at[other], core_r.at[5])
    arrived(t0recv, core_r.at[2])
    for h in range(heads):
        back = gall[h // 2, col(h % 2), :].astype(F32) + jnp.where(c == 0, t0recv[col(h), :].astype(F32), 0.0)
        back = back.astype(BF16)
        kg_ref[:, col(h)] = (kgl[:, col(h)] + mm(v_ref[:, col(h)], back, NT)).astype(BF16)
        vg_ref[:, col(h)] = (vgl[:, col(h)] + mm(k_ref[:, col(h)], back, NN)).astype(BF16)

    arrived(mrecv.at[0], m_r.at[2])
    arrived(mrecv.at[1], m_r.at[3])
    mixed_ref[...] = (
        mpart[y].astype(F32) + mrecv[0].astype(F32) + mrecv[1].astype(F32)
    ).astype(BF16)

    for off in range(1, NX):
        arrived(tgx.at[mod(x - off, NX)], tx_r.at[off])
    table = tgx[0]
    for xs in range(1, NX):
        table = table + tgx[xs]
    tokens = rows * 2 * NZ * NX
    square = jnp.concatenate([table, jnp.zeros((size - CODES, size), F32)], axis=0)
    tg_ref[...] = square.T[:heads, :CODES] * (1.0 / math.sqrt(tokens * levels))

    for i in range(PIECES):
        for off in range(1, NZ):
            arrived(wzrecv.at[mod(z - off, NZ), :, sides[i]], wz_r.at[off, i])
        weight = wzrecv[0, :, sides[i]].astype(F32)
        for zs in range(1, NZ):
            weight = weight + wzrecv[zs, :, sides[i]].astype(F32)
        wg_ref[:, sides[i]] = weight * (1.0 / math.sqrt(tokens))

    for copy, cond in pending:
        if cond is None:
            copy.wait_send()
        else:
            pl.when(cond)(lambda copy=copy: copy.wait_send())


def store(*refs):
    sources, targets, sems = refs[:6], refs[6:12], refs[12]
    copies = [
        pltpu.make_async_copy(source, target, sems.at[i])
        for i, (source, target) in enumerate(zip(sources, targets))
    ]
    for copy in copies:
        copy.start()
    for copy in copies:
        copy.wait()


def per_device(queries, keys, values, level_table, level_code, out_weight, cotangent):
    rows, width = queries.shape
    vmem = pl.BlockSpec(memory_space=pltpu.VMEM)
    hbm = pl.BlockSpec(memory_space=pltpu.MemorySpace.HBM)
    dma = pltpu.SemaphoreType.DMA

    def bf(*shape):
        return pltpu.VMEM(shape, BF16)

    def f32(*shape):
        return pltpu.VMEM(shape, F32)

    scratch = [
        bf(rows, 512), bf(rows, 512), bf(rows, 512), bf(512, 2048), dma((5,)),
        pltpu.SemaphoreType.REGULAR((2,)), f32(4, rows, 768), bf(4, rows, 512), f32(4, 6, rows, 128), f32(4, rows, rows), f32(4, rows, rows),
        bf(4, rows, rows), bf(4, rows, 768), bf(rows, 512), bf(rows, 512),
        f32(rows, 512), f32(rows, 512), f32(rows, 512), f32(rows, 512),
        bf(512, 128), bf(512, 128), bf(256, 128), bf(NZ, 32, 128), bf(32, 128), bf(NX, 32, 128),
        bf(NZ, 3, 32, 128), bf(2, 32, 128), bf(5, 2, 256, 128),
        bf(512, 128), bf(512, 128), bf(5, 2, 256, 128), bf(5, 256, 128), bf(5, 256, 128),
        bf(NZ, 5, 32, 128), bf(2, 32, 128), bf(NX, 32, 128), bf(NZ, 32, 128), bf(2, 256, 128),
        bf(4, rows, 512), bf(2, rows // 2, 512), bf(2, rows, 512),
        bf(4, 2, 256, 512), bf(4, 256, 512), bf(2, 128, 512), bf(2, 256, 512), bf(256, 512),
        bf(NZ, 32, 512),
        f32(CODES, 128), f32(CODES, 128), f32(CODES, 128), f32(NZ, CODES, 128),
        f32(CODES, 128), f32(NX, CODES, 128),
        dma((6,)), dma((6,)), dma((6,)), dma((6,)), dma((NZ,)), dma((NZ,)), dma((NX,)), dma((NX,)),
        dma((NZ, 5)), dma((NZ, 5)), dma((NZ, 5)), dma((NZ, 5)), dma((NX,)), dma((NX,)),
        dma((NZ,)), dma((NZ,)), dma((4,)), dma((4,)), dma((4,)), dma((4,)), dma((4 * PIECES,)), dma((4 * PIECES,)),
        dma((NZ, PIECES)), dma((NZ, PIECES)), dma((NZ,)), dma((NZ,)), dma((NX,)), dma((NX,)),
    ]
    shape = jax.ShapeDtypeStruct
    results = pl.pallas_call(
        kernel,
        out_shape=(
            shape((rows, width), BF16),
            shape((32, width), F32),
            shape((rows, width), BF16),
            shape((rows, width), BF16),
            shape((rows, width), BF16),
            shape((4, CODES), F32),
        ),
        in_specs=[hbm, hbm, hbm, vmem, vmem, hbm, hbm],
        out_specs=[vmem] * 6,
        scratch_shapes=scratch,
        compiler_params=pltpu.CompilerParams(
            collective_id=0, has_side_effects=True, vmem_limit_bytes=53900 * 2**10
        ),
        name="layer",
    )(queries, keys, values, level_table.T, level_code.T, out_weight, cotangent)
    stored = pl.pallas_call(
        store,
        out_shape=tuple(shape(value.shape, value.dtype) for value in results),
        in_specs=[vmem] * 6,
        out_specs=[pl.BlockSpec(memory_space=pl.ANY)] * 6,
        scratch_shapes=[dma((6,))],
        compiler_params=pltpu.CompilerParams(vmem_limit_bytes=2**20),
        name="store",
    )(*results)
    return (*stored[:5], stored[5].T)


def solution(mesh):
    wide = P("seq", "head")
    return jax.shard_map(
        per_device,
        mesh=mesh,
        in_specs=(wide, wide, wide, P(None, "head"), P("seq", None), P("head", None), wide),
        out_specs=(wide, wide, wide, wide, wide, P(None, "head")),
        check_vma=False,
    )
```

```python
import math

import jax
import jax.numpy as jnp
from jax import lax
from jax.experimental import pallas as pl
from jax.experimental.pallas import tpu as pltpu
from jax.sharding import PartitionSpec as P

SPAN = 64
CODES = 16
NX, NZ = 4, 8
Z_ORDER = (4, 3, 5, 2, 6, 1, 7)
PIECES = 4
F32, BF16 = jnp.float32, jnp.bfloat16
MESH = pl.DeviceIdType.MESH
NN = (((1,), (0,)), ((), ()))
NT = (((1,), (1,)), ((), ()))
TN = (((0,), (0,)), ((), ()))


def mm(left, right, dims):
    return lax.dot_general(left, right, dims, preferred_element_type=F32)


def remote(src, dst, send_sem, recv_sem, device):
    return pltpu.make_async_remote_copy(
        src_ref=src,
        dst_ref=dst,
        send_sem=send_sem,
        recv_sem=recv_sem,
        device_id=device,
        device_id_type=MESH,
    )


def mod(value, size):
    return lax.rem(value + size, size)


def bit_of(value, index):
    return lax.rem(lax.div(value, 2**index), 2)


def kernel(
    q_hbm, k_hbm, v_hbm, table_ref, code_ref, w_hbm, cot_hbm,
    mixed_ref, wg_ref, qg_ref, kg_ref, vg_ref, tg_ref,
    q_ref, k_ref, v_ref, w_ref, load_sems, far_sems, reads, cotall, coefb, scores, lw, probs, sgbuf, gbuf, abuf, attnl, qgl, kgl, vgl,
    dsend, drecv, zsend_f, zrecv_f, xsend_f, xrecv_f, rsend_f, rx_f, fall,
    t0send, t0recv, tsend, trecv, zsend_b, zrecv_b, xsend_b, xrecv_b, gsend, gall,
    mpart, mrelay, mrecv, wpart, wrecv, wrelay, wxrecv, wz, wzrecv,
    tgsend, tgcore, tgzsend, tgz, tgxsend, tgx,
    cot_s, cot_r, core_s, core_r, zf_s, zf_r, xf_s, xf_r, rf_s, rf_r,
    zb_s, zb_r, xb_s, xb_r, rb_s, rb_r, m_s, m_r, wc_s, wc_r, wx_s, wx_r, wz_s, wz_r,
    tz_s, tz_r, tx_s, tx_r,
):
    s = lax.axis_index("seq")
    y = lax.axis_index("head")
    c = lax.rem(s, 2)
    z = lax.rem(lax.div(s, 2), NZ)
    x = lax.div(s, 2 * NZ)
    other = 1 - c
    heads, size = 4, 128
    rows = q_ref.shape[0]
    loads = [
        pltpu.make_async_copy(source, target, load_sems.at[i])
        for i, (source, target) in enumerate(
            [(cot_hbm, cotall.at[y]), (k_hbm, k_ref), (v_hbm, v_ref), (q_hbm, q_ref), (w_hbm, w_ref)]
        )
    ]
    for load in loads:
        load.start()
    half = rows // 2

    def at_y(target):
        return (s, target)

    def at_z(target):
        return ((x * NZ + target) * 2 + c, y)

    def at_x(target):
        return ((target * NZ + z) * 2 + c, y)

    partner = (s + 1 - 2 * c, y)
    level_bits = [bit_of(z, 0), bit_of(z, 1), bit_of(z, 2), bit_of(x, 0), bit_of(x, 1)]
    pending = []

    def go(copy, cond=None):
        pending.append((copy, cond))
        if cond is None:
            copy.start()
        else:
            pl.when(cond)(lambda: copy.start())

    def arrived(dst, sem, cond=None):
        copy = remote(dst, dst, sem, sem, partner)
        if cond is None:
            copy.wait_recv()
        else:
            pl.when(cond)(lambda: copy.wait_recv())

    def col(h):
        return slice(h * size, (h + 1) * size)

    right, left = mod(y + 1, 4), mod(y - 1, 4)
    x_right, x_left, x_opposite = mod(x + 1, 4), mod(x - 1, 4), mod(x + 2, 4)
    barrier = pltpu.get_barrier_semaphore()
    near = [partner, at_y(right), at_y(left), at_x(x_right), at_x(x_left), at_x(x_opposite)]
    near += [at_z(mod(z + off, NZ)) for off in (1, -1, 2, -2)]
    for device in near:
        pl.semaphore_signal(barrier, inc=1, device_id=device, device_id_type=MESH)

    def tell(index, device):
        pl.semaphore_signal(far_sems.at[index], inc=1, device_id=device, device_id_type=MESH)

    def tell_z():
        tell(0, at_z(mod(z + 2, NZ)))
        tell(1, at_z(mod(z - 2, NZ)))

    def hear_z():
        pl.semaphore_wait(far_sems.at[0], 1)
        pl.semaphore_wait(far_sems.at[1], 1)

    loads[1].wait()
    loads[2].wait()
    for h in range(heads):
        dsend[col(h), :] = mm(k_ref[:, col(h)], v_ref[:, col(h)], TN).astype(BF16)
    for l in range(5):
        @pl.when(level_bits[l] == 0)
        def _(l=l):
            fall[l, c] = jnp.zeros((256, size), BF16)
    loads[0].wait()
    pl.semaphore_wait(barrier, len(near))

    top, low = pl.ds(0, half), pl.ds(half, half)
    go(remote(cotall.at[y, top], cotall.at[y, top], cot_s.at[0], cot_r.at[0], at_y(right)))
    go(remote(cotall.at[y, low], cotall.at[y, low], cot_s.at[2], cot_r.at[2], at_y(left)))
    go(remote(cotall.at[y, low], cotall.at[y, low], cot_s.at[1], cot_r.at[1], at_y(right)))
    go(remote(cotall.at[y, top], cotall.at[y, top], cot_s.at[3], cot_r.at[3], at_y(left)))
    go(remote(dsend, drecv, core_s.at[0], core_r.at[0], partner))
    tell_z()

    levels = code_ref.shape[0]
    code_t = code_ref[...].astype(F32)
    padding = jnp.zeros((size - levels, rows), F32)
    code = jnp.concatenate([code_t, padding], axis=0).T
    lane = lax.broadcasted_iota(jnp.int32, (1, size), 1)
    scale = jnp.zeros((1, size), F32)
    scales = [1.0 / math.sqrt(SPAN * 2 ** max(l - 1, 0)) for l in range(levels)]
    for l in range(levels):
        scale = jnp.where(lane == l, scales[l], scale)
    coefs = []
    for h in range(heads):
        lam = jnp.zeros((rows, size), F32)
        for entry in range(CODES):
            lam = jnp.where(code == float(entry), table_ref[h:h + 1, entry:entry + 1], lam)
        coefs.append(lam * scale)

    loads[3].wait()
    row = lax.broadcasted_iota(jnp.int32, (rows, rows), 0)
    column = lax.broadcasted_iota(jnp.int32, (rows, rows), 1)
    row_span, column_span = row // SPAN, column // SPAN
    in_level = [
        (row_span == column_span) & (column <= row),
        (row_span // 2 == column_span // 2) & (column_span < row_span),
        (row_span >= 2) & (column_span < 2),
    ]

    def local_forward(h):
        weight = jnp.zeros((rows, rows), F32)
        for l in range(3):
            weight = jnp.where(in_level[l], coefs[h][:, l:l + 1], weight)
        score = mm(q_ref[:, col(h)], k_ref[:, col(h)], NT)
        scores[h] = score
        lw[h] = weight
        prob = (score * weight).astype(BF16)
        probs[h] = prob
        attnl[:, col(h)] = mm(prob, v_ref[:, col(h)], NN)

    for h in range(2):
        local_forward(h)
    arrived(drecv, core_r.at[0])
    half_rows = pl.ds(pl.multiple_of(c * 256, 256), 256)
    zsend_f[...] = (dsend[half_rows, :].astype(F32) + drecv[half_rows, :].astype(F32)).astype(BF16)
    hear_z()
    for off in Z_ORDER:
        zt = mod(z + off, NZ)
        go(remote(zsend_f.at[pl.ds(pl.multiple_of(zt * 32, 32), 32)], zrecv_f.at[z],
                  zf_s.at[off], zf_r.at[off], at_z(zt)))
    own_slice = pl.ds(pl.multiple_of(z * 32, 32), 32)
    zrecv_f[z] = zsend_f[own_slice, :]

    for h in range(2, heads):
        local_forward(h)
    for h in range(heads):
        for l in range(3, levels):
            coefb[h, l - 3] = jnp.broadcast_to(coefs[h][:, l:l + 1], (rows, size))

    arrived(cotall.at[left, top], cot_r.at[0])
    go(remote(cotall.at[left, top], cotall.at[left, top], cot_s.at[4], cot_r.at[4], at_y(right)))
    arrived(cotall.at[right, low], cot_r.at[2])
    go(remote(cotall.at[right, low], cotall.at[right, low], cot_s.at[5], cot_r.at[5], at_y(left)))

    for off in range(1, NZ):
        arrived(zrecv_f.at[mod(z - off, NZ)], zf_r.at[off])
    parts = [zrecv_f[i].astype(F32) for i in range(NZ)]
    pairs = [parts[2 * i] + parts[2 * i + 1] for i in range(4)]
    quads = [pairs[0] + pairs[1], pairs[2] + pairs[3]]
    xsend_f[...] = (quads[0] + quads[1]).astype(BF16)
    for off in range(1, NX):
        xt = mod(x + off, NX)
        go(remote(xsend_f, xrecv_f.at[x], xf_s.at[off], xf_r.at[off], at_x(xt)), xt > x)
    for zt in range(NZ):
        if zt & 1:
            rsend_f[zt, 0] = parts[zt - 1].astype(BF16)
        if zt & 2:
            rsend_f[zt, 1] = pairs[2 * (zt // 4)].astype(BF16)
        if zt & 4:
            rsend_f[zt, 2] = quads[0].astype(BF16)
    for off in Z_ORDER:
        zt = mod(z + off, NZ)
        for l in range(3):
            go(remote(rsend_f.at[zt, l], fall.at[l, c, own_slice],
                      rf_s.at[off, l], rf_r.at[off, l], at_z(zt)), bit_of(zt, l) == 1)
    for l in range(3):
        @pl.when(level_bits[l] == 1)
        def _(l=l):
            fall[l, c, own_slice, :] = rsend_f[z, l]

    for off in range(1, NX):
        xs = mod(x - off, NX)
        arrived(xrecv_f.at[xs], xf_r.at[off], xs < x)

    @pl.when(bit_of(x, 0) == 1)
    def _():
        rx_f[0] = xrecv_f[x - 1]
        fall[3, c, own_slice, :] = xrecv_f[x - 1]

    @pl.when(x >= 2)
    def _():
        both = (xrecv_f[0].astype(F32) + xrecv_f[1].astype(F32)).astype(BF16)
        rx_f[1] = both
        fall[4, c, own_slice, :] = both

    for off in Z_ORDER:
        zt = mod(z + off, NZ)
        for l in range(3, 5):
            go(remote(rx_f.at[l - 3], fall.at[l, c, own_slice],
                      rf_s.at[off, l], rf_r.at[off, l], at_z(zt)), level_bits[l] == 1)

    loads[4].wait()
    opposite = mod(y + 2, 4)
    arrived(cotall.at[left, low], cot_r.at[1])
    arrived(cotall.at[right, top], cot_r.at[3])
    arrived(cotall.at[opposite, top], cot_r.at[4])
    arrived(cotall.at[opposite, low], cot_r.at[5])
    full_rows = jnp.concatenate([cotall[i] for i in range(4)], axis=1)
    gbuf[...] = mm(full_rows, w_ref[...], NT).astype(BF16)

    for h in range(heads):
        grad = gbuf[:, col(h)].astype(F32)
        for l in range(6):
            sgbuf[h, :, col(l)] = (coefb[h, l] * grad).astype(BF16)
        terms = mm(q_ref[:, col(h)], sgbuf[h], TN)
        t0send[col(h), :] = terms[:, col(0)].astype(BF16)
        for l in range(5):
            tsend[l, h // 2, col(h % 2), :] = terms[:, col(l + 1)].astype(BF16)
    go(remote(tsend.at[:, other], trecv, core_s.at[1], core_r.at[1], partner))
    go(remote(t0send, t0recv, core_s.at[2], core_r.at[2], partner))

    for off in range(1, NZ):
        zs = mod(z - off, NZ)
        zs_slice = pl.ds(pl.multiple_of(zs * 32, 32), 32)
        for l in range(5):
            arrived(fall.at[l, c, zs_slice], rf_r.at[off, l], level_bits[l] == 1)
    go(remote(fall.at[:, c], fall.at[:, c], core_s.at[3], core_r.at[3], partner))

    arrived(trecv, core_r.at[1])
    for l in range(5):
        zsend_b[l] = (tsend[l, c].astype(F32) + trecv[l].astype(F32)).astype(BF16)
    for off in Z_ORDER:
        zt = mod(z + off, NZ)
        for l in range(5):
            go(remote(zsend_b.at[l, pl.ds(pl.multiple_of(zt * 32, 32), 32)], zrecv_b.at[z, l],
                      zb_s.at[off, l], zb_r.at[off, l], at_z(zt)), level_bits[l] == 1)
    for l in range(5):
        @pl.when(level_bits[l] == 1)
        def _(l=l):
            zrecv_b[z, l] = zsend_b[l, own_slice, :]

    arrived(fall.at[:, other], core_r.at[3])

    def found_states(h):
        found = [jnp.where(c == 1, drecv[col(h), :], jnp.zeros((size, size), BF16))]
        found += [fall[l, h // 2, col(h % 2), :] for l in range(5)]
        return jnp.concatenate(found, axis=1)

    for h in range(heads):
        values = mm(q_ref[:, col(h)], found_states(h), NN)
        reads[h] = values
        attention = attnl[:, col(h)]
        for l in range(6):
            attention = attention + coefb[h, l] * values[:, col(l)]
        abuf[:, col(h)] = attention.astype(BF16)

    def weight_part(step, target):
        part = mm(cotall[target], abuf[...], TN)
        for block in range(16):
            wpart[target, block % 2, pl.ds((block // 2) * 32, 32), :] = (
                part[block * 32:(block + 1) * 32].astype(BF16)
            )
        go(remote(wpart.at[target, other], wrecv.at[target], wc_s.at[step], wc_r.at[step], partner))

    def weight_chip(step, target):
        arrived(wrecv.at[target], wc_r.at[step])
        wpart[target, c] = (wpart[target, c].astype(F32) + wrecv[target].astype(F32)).astype(BF16)

    def product_for(target):
        columns = pl.ds(pl.multiple_of(target * 512, 512), 512)
        mpart[target] = mm(abuf[...], w_ref[:, columns], NN).astype(BF16)

    sides = [pl.ds(128 * i, 128) for i in range(PIECES)]
    weight_part(0, x_opposite)
    weight_part(1, x_left)
    weight_chip(0, x_opposite)
    for i in range(PIECES):
        go(remote(wpart.at[x_opposite, c, top, sides[i]], wrelay.at[0, :, sides[i]],
                  wx_s.at[4 * i], wx_r.at[4 * i], at_x(x_left)))
        go(remote(wpart.at[x_opposite, c, low, sides[i]], wrelay.at[1, :, sides[i]],
                  wx_s.at[4 * i + 1], wx_r.at[4 * i + 1], at_x(x_right)))
    product_for(opposite)
    go(remote(mpart.at[opposite, top], mrelay.at[0], m_s.at[0], m_r.at[0], at_y(left)))
    go(remote(mpart.at[opposite, low], mrelay.at[1], m_s.at[1], m_r.at[1], at_y(right)))
    weight_part(2, x_right)
    product_for(left)
    product_for(right)
    entry_row = lax.broadcasted_iota(jnp.int32, (CODES, rows), 0).astype(F32)
    one_hot = [
        jnp.where(jnp.broadcast_to(code_t[l:l + 1, :], (CODES, rows)) == entry_row, 1.0, 0.0).astype(BF16)
        for l in range(levels)
    ]
    table_parts = []

    def local_back(h):
        grad = gbuf[:, col(h)]
        prob_grad = mm(grad, v_ref[:, col(h)], NT)
        score_grad = (prob_grad * lw[h]).astype(BF16)
        product = scores[h] * prob_grad
        total = jnp.zeros((CODES, rows), F32)
        for l in range(3):
            masked = jnp.where(in_level[l], product, 0.0).astype(BF16)
            total = total + scales[l] * mm(one_hot[l], masked, NN)
        qgl[:, col(h)] = mm(score_grad, k_ref[:, col(h)], NN)
        kgl[:, col(h)] = mm(score_grad, q_ref[:, col(h)], TN)
        vgl[:, col(h)] = mm(probs[h], grad, TN)
        table_parts.append(total[:, :size] + total[:, size:])

    for h in range(3):
        local_back(h)

    weight_chip(1, x_left)
    weight_chip(2, x_right)

    def weight_relay(i):
        side = sides[i]
        arrived(wrelay.at[0, :, side], wx_r.at[4 * i])
        wpart[x_left, c, top, side] = (
            wpart[x_left, c, top, side].astype(F32) + wrelay[0, :, side].astype(F32)
        ).astype(BF16)
        go(remote(wpart.at[x_left, c, :, side], wxrecv.at[0, :, side],
                  wx_s.at[4 * i + 2], wx_r.at[4 * i + 2], at_x(x_left)))
        arrived(wrelay.at[1, :, side], wx_r.at[4 * i + 1])
        wpart[x_right, c, low, side] = (
            wpart[x_right, c, low, side].astype(F32) + wrelay[1, :, side].astype(F32)
        ).astype(BF16)
        go(remote(wpart.at[x_right, c, :, side], wxrecv.at[1, :, side],
                  wx_s.at[4 * i + 3], wx_r.at[4 * i + 3], at_x(x_right)))

    weight_relay(0)
    for off in range(1, NZ):
        zs = mod(z - off, NZ)
        for l in range(5):
            bit = bit_of(zs, l) if l < 3 else level_bits[l]
            arrived(zrecv_b.at[zs, l], zb_r.at[off, l], bit == 1)
    for l in range(2):
        @pl.when(level_bits[3 + l] == 1)
        def _(l=l):
            ring = zrecv_b[0, 3 + l].astype(F32)
            for zs in range(1, NZ):
                ring = ring + zrecv_b[zs, 3 + l].astype(F32)
            xsend_b[l] = ring.astype(BF16)
    for off in range(1, NX):
        xt = mod(x + off, NX)
        bit = jnp.where(lax.div(x, 2) == lax.div(xt, 2), 0, 1)
        go(remote(xsend_b.at[bit], xrecv_b.at[x], xb_s.at[off], xb_r.at[off], at_x(xt)), xt < x)

    local_back(3)
    weight_relay(1)
    for h in range(heads):
        grad = gbuf[:, col(h)].astype(F32)
        total = table_parts[h]
        for l in range(6):
            total = total + scales[l + 3] * mm(one_hot[l + 3], (grad * reads[h, :, col(l)]).astype(BF16), NN)
        table_parts[h] = total
    lane128 = lax.broadcasted_iota(jnp.int32, (CODES, size), 1)
    partial_table = jnp.zeros((CODES, size), F32)
    for h in range(heads):
        summed = jnp.sum(table_parts[h], axis=1, keepdims=True)
        partial_table = jnp.where(lane128 == h, summed, partial_table)
    tgsend[...] = partial_table
    go(remote(tgsend, tgcore, core_s.at[4], core_r.at[4], partner))

    for i in range(2, PIECES):
        weight_relay(i)

    weight_part(3, x)
    product_for(y)
    for off in range(1, NX):
        xs = mod(x - off, NX)
        arrived(xrecv_b.at[xs], xb_r.at[off], xs > x)
    from_x = jnp.zeros((32, size), F32)
    for xs in range(1, NX):
        from_x = from_x + jnp.where(x < xs, xrecv_b[xs].astype(F32), 0.0)
    quad = zrecv_b[4, 2].astype(F32)
    for zs in range(5, NZ):
        quad = quad + zrecv_b[zs, 2].astype(F32)
    for zt in range(NZ):
        total = from_x
        if zt & 1 == 0:
            total = total + zrecv_b[zt + 1, 0].astype(F32)
        if zt & 2 == 0:
            upper = (zt // 4) * 4 + 2
            total = total + zrecv_b[upper, 1].astype(F32) + zrecv_b[upper + 1, 1].astype(F32)
        if zt & 4 == 0:
            total = total + quad
        gsend[zt] = total.astype(BF16)
    for off in Z_ORDER:
        zt = mod(z + off, NZ)
        go(remote(gsend.at[zt], gall.at[c, own_slice], rb_s.at[off], rb_r.at[off], at_z(zt)))
    gall[c, own_slice, :] = gsend[z]

    arrived(tgcore, core_r.at[4])
    tgzsend[...] = tgsend[...] + tgcore[...]
    for off in range(1, NZ):
        go(remote(tgzsend, tgz.at[z], tz_s.at[off], tz_r.at[off], at_z(mod(z + off, NZ))))
    tgz[z] = tgzsend[...]

    def weight_ring(i):
        side = sides[i]
        arrived(wxrecv.at[0, :, side], wx_r.at[4 * i + 2])
        arrived(wxrecv.at[1, :, side], wx_r.at[4 * i + 3])
        wz[:, side] = (
            wpart[x, c, :, side].astype(F32) + wxrecv[0, :, side].astype(F32) + wxrecv[1, :, side].astype(F32)
        ).astype(BF16)
        for off in Z_ORDER:
            zt = mod(z + off, NZ)
            go(remote(wz.at[pl.ds(pl.multiple_of(zt * 32, 32), 32), side], wzrecv.at[z, :, side],
                      wz_s.at[off, i], wz_r.at[off, i], at_z(zt)))
        wzrecv[z, :, side] = wz[own_slice, side]

    weight_chip(3, x)
    weight_ring(0)
    arrived(mrelay.at[0], m_r.at[0])
    mpart[left, top] = (mpart[left, top].astype(F32) + mrelay[0].astype(F32)).astype(BF16)
    go(remote(mpart.at[left], mrecv.at[0], m_s.at[2], m_r.at[2], at_y(left)))
    arrived(mrelay.at[1], m_r.at[1])
    mpart[right, low] = (mpart[right, low].astype(F32) + mrelay[1].astype(F32)).astype(BF16)
    go(remote(mpart.at[right], mrecv.at[1], m_s.at[3], m_r.at[3], at_y(right)))

    weight_ring(1)
    for h in range(heads):
        qg_ref[:, col(h)] = (qgl[:, col(h)] + mm(sgbuf[h], found_states(h), NT)).astype(BF16)
    for i in range(2, PIECES):
        weight_ring(i)

    for off in range(1, NZ):
        zs = mod(z - off, NZ)
        arrived(gall.at[c, pl.ds(pl.multiple_of(zs * 32, 32), 32)], rb_r.at[off])
    go(remote(gall.at[c], gall.at[c], core_s.at[5], core_r.at[5], partner))
    for off in range(1, NZ):
        arrived(tgz.at[mod(z - off, NZ)], tz_r.at[off])
    ring_table = tgz[0]
    for zs in range(1, NZ):
        ring_table = ring_table + tgz[zs]
    tgxsend[...] = ring_table
    for off in range(1, NX):
        go(remote(tgxsend, tgx.at[x], tx_s.at[off], tx_r.at[off], at_x(mod(x + off, NX))))
    tgx[x] = ring_table

    arrived(gall.at[other], core_r.at[5])
    arrived(t0recv, core_r.at[2])
    for h in range(heads):
        back = gall[h // 2, col(h % 2), :].astype(F32) + jnp.where(c == 0, t0recv[col(h), :].astype(F32), 0.0)
        back = back.astype(BF16)
        kg_ref[:, col(h)] = (kgl[:, col(h)] + mm(v_ref[:, col(h)], back, NT)).astype(BF16)
        vg_ref[:, col(h)] = (vgl[:, col(h)] + mm(k_ref[:, col(h)], back, NN)).astype(BF16)

    arrived(mrecv.at[0], m_r.at[2])
    arrived(mrecv.at[1], m_r.at[3])
    mixed_ref[...] = (
        mpart[y].astype(F32) + mrecv[0].astype(F32) + mrecv[1].astype(F32)
    ).astype(BF16)

    for off in range(1, NX):
        arrived(tgx.at[mod(x - off, NX)], tx_r.at[off])
    table = tgx[0]
    for xs in range(1, NX):
        table = table + tgx[xs]
    tokens = rows * 2 * NZ * NX
    square = jnp.concatenate([table, jnp.zeros((size - CODES, size), F32)], axis=0)
    tg_ref[...] = square.T[:heads, :CODES] * (1.0 / math.sqrt(tokens * levels))

    for i in range(PIECES):
        for off in range(1, NZ):
            arrived(wzrecv.at[mod(z - off, NZ), :, sides[i]], wz_r.at[off, i])
        weight = wzrecv[0, :, sides[i]].astype(F32)
        for zs in range(1, NZ):
            weight = weight + wzrecv[zs, :, sides[i]].astype(F32)
        wg_ref[:, sides[i]] = weight * (1.0 / math.sqrt(tokens))

    for copy, cond in pending:
        if cond is None:
            copy.wait_send()
        else:
            pl.when(cond)(lambda copy=copy: copy.wait_send())


def store(*refs):
    sources, targets, sems = refs[:6], refs[6:12], refs[12]
    copies = [
        pltpu.make_async_copy(source, target, sems.at[i])
        for i, (source, target) in enumerate(zip(sources, targets))
    ]
    for copy in copies:
        copy.start()
    for copy in copies:
        copy.wait()


def per_device(queries, keys, values, level_table, level_code, out_weight, cotangent):
    rows, width = queries.shape
    vmem = pl.BlockSpec(memory_space=pltpu.VMEM)
    hbm = pl.BlockSpec(memory_space=pltpu.MemorySpace.HBM)
    dma = pltpu.SemaphoreType.DMA

    def bf(*shape):
        return pltpu.VMEM(shape, BF16)

    def f32(*shape):
        return pltpu.VMEM(shape, F32)

    scratch = [
        bf(rows, 512), bf(rows, 512), bf(rows, 512), bf(512, 2048), dma((5,)),
        pltpu.SemaphoreType.REGULAR((2,)), f32(4, rows, 768), bf(4, rows, 512), f32(4, 6, rows, 128), f32(4, rows, rows), f32(4, rows, rows),
        bf(4, rows, rows), bf(4, rows, 768), bf(rows, 512), bf(rows, 512),
        f32(rows, 512), f32(rows, 512), f32(rows, 512), f32(rows, 512),
        bf(512, 128), bf(512, 128), bf(256, 128), bf(NZ, 32, 128), bf(32, 128), bf(NX, 32, 128),
        bf(NZ, 3, 32, 128), bf(2, 32, 128), bf(5, 2, 256, 128),
        bf(512, 128), bf(512, 128), bf(5, 2, 256, 128), bf(5, 256, 128), bf(5, 256, 128),
        bf(NZ, 5, 32, 128), bf(2, 32, 128), bf(NX, 32, 128), bf(NZ, 32, 128), bf(2, 256, 128),
        bf(4, rows, 512), bf(2, rows // 2, 512), bf(2, rows, 512),
        bf(4, 2, 256, 512), bf(4, 256, 512), bf(2, 128, 512), bf(2, 256, 512), bf(256, 512),
        bf(NZ, 32, 512),
        f32(CODES, 128), f32(CODES, 128), f32(CODES, 128), f32(NZ, CODES, 128),
        f32(CODES, 128), f32(NX, CODES, 128),
        dma((6,)), dma((6,)), dma((6,)), dma((6,)), dma((NZ,)), dma((NZ,)), dma((NX,)), dma((NX,)),
        dma((NZ, 5)), dma((NZ, 5)), dma((NZ, 5)), dma((NZ, 5)), dma((NX,)), dma((NX,)),
        dma((NZ,)), dma((NZ,)), dma((4,)), dma((4,)), dma((4,)), dma((4,)), dma((4 * PIECES,)), dma((4 * PIECES,)),
        dma((NZ, PIECES)), dma((NZ, PIECES)), dma((NZ,)), dma((NZ,)), dma((NX,)), dma((NX,)),
    ]
    shape = jax.ShapeDtypeStruct
    results = pl.pallas_call(
        kernel,
        out_shape=(
            shape((rows, width), BF16),
            shape((32, width), F32),
            shape((rows, width), BF16),
            shape((rows, width), BF16),
            shape((rows, width), BF16),
            shape((4, CODES), F32),
        ),
        in_specs=[hbm, hbm, hbm, vmem, vmem, hbm, hbm],
        out_specs=[vmem] * 6,
        scratch_shapes=scratch,
        compiler_params=pltpu.CompilerParams(
            collective_id=0, has_side_effects=True, vmem_limit_bytes=53900 * 2**10
        ),
        name="layer",
    )(queries, keys, values, level_table.T, level_code.T, out_weight, cotangent)
    stored = pl.pallas_call(
        store,
        out_shape=tuple(shape(value.shape, value.dtype) for value in results),
        in_specs=[vmem] * 6,
        out_specs=[pl.BlockSpec(memory_space=pl.ANY)] * 6,
        scratch_shapes=[dma((6,))],
        compiler_params=pltpu.CompilerParams(vmem_limit_bytes=2**20),
        name="store",
    )(*results)
    return (*stored[:5], stored[5].T)


def solution(mesh):
    wide = P("seq", "head")
    return jax.shard_map(
        per_device,
        mesh=mesh,
        in_specs=(wide, wide, wide, P(None, "head"), P("seq", None), P("head", None), wide),
        out_specs=(wide, wide, wide, wide, wide, P(None, "head")),
        check_vma=False,
    )
```
